128 devices in a mesh: seq: 32 (over z, x, y_hi), tp: 4 (over y_lo, core).
Axes of the slice: x: 4, y: 4 (y_hi: 2, y_lo: 2; y = y_hi * 2 + y_lo), z: 4, core: 2. Of those that a mesh axis runs over, the one named last changes fastest.
Arguments:
- queries: bfloat16 [65536, 2048], P('seq', 'tp'), may hold values from -6 to 6
- key_vectors: bfloat16 [65536, 2048], P('seq', 'tp'), may hold values from -6 to 6
- value_vectors: bfloat16 [65536, 2048], P('seq', 'tp'), may hold values from -6 to 6
- out_grad: bfloat16 [65536, 2048], P('seq', 'tp'), may hold values from -0.25 to 0.25
- log_decay: float32 [8, 65536], P(None, 'seq'), may hold values from -2 to 0, as said below
- inputs: bfloat16 [65536, 2048], P('seq'), may hold values from -0.109375 to 0.109375
Outputs:
- key_grad: bfloat16 [65536, 2048], P('seq', 'tp')
- value_grad: bfloat16 [65536, 2048], P('seq', 'tp')
- weight_grad: bfloat16 [2048, 2, 2048], P('seq', None, 'tp')
The draws below stay inside these ranges and needn't reach their ends.
Inputs may be any that keep to these rules, and one draw needn't show every extreme that they name: `log_decay`: every entry is negative.
All inputs are finite; a program needn't handle non-finite values.
Results may differ from the reference program's by a relative error of at most 0.0066.
Values may be sent and summed in bfloat16 or wider, within the bound.
No kernel may reach another device: no remote copies, remote signals or barrier semaphores. Data moves between devices by JAX's collectives and lax.ppermute only.
A program may use at most 128 MiB of HBM per device.

```python
import math
import jax
import jax.numpy as jnp
from jax import lax

D = 2048
H = 8
DH = 256
BLOCK = 512
SEQUENCE_TOKENS = 65536


def draw_log_decay(key, part):
    random_subkeys = jax.random.split(key, 7)
    ordering = jax.random.permutation(random_subkeys[0], H)
    slow_heads = ordering >= H // 2
    fast_rate = jnp.exp(jax.random.uniform(random_subkeys[1], (H,), jnp.float32, math.log(1.0 / 50.0), math.log(1.0 / 30.0)))
    slow_rate = jnp.exp(jax.random.uniform(random_subkeys[2], (H,), jnp.float32, math.log(0.05 / SEQUENCE_TOKENS), math.log(0.3 / SEQUENCE_TOKENS)))
    base_rate = jnp.where(slow_heads, slow_rate, fast_rate)
    block_count = SEQUENCE_TOKENS // BLOCK
    block_factor = jnp.exp(jax.random.uniform(random_subkeys[3], (H, block_count), jnp.float32, math.log(0.5), math.log(2.0)))
    roughness = jax.random.uniform(random_subkeys[4], (H, SEQUENCE_TOKENS), jnp.float32, 0.5, 1.5)
    decay_speeds = base_rate[:, None] * jnp.repeat(block_factor, BLOCK, axis=1) * roughness
    spike_location = jax.random.randint(random_subkeys[5], (2,), 0, SEQUENCE_TOKENS)
    spike_amplitude = jnp.log(jax.random.uniform(random_subkeys[6], (2,), jnp.float32, 0.5, 0.8))
    token_offsets = jnp.arange(SEQUENCE_TOKENS)
    spike_events = jnp.where(token_offsets == spike_location[0], spike_amplitude[0], 0.0) + jnp.where(token_offsets == spike_location[1], spike_amplitude[1], 0.0)
    return -decay_speeds + spike_events[None, :]


def spiked(values, rng, source, target, shards_of, factor):
    def block_of(position):
        return (jnp.arange(values.shape[position]) // (values.shape[position] // shards_of)).reshape((-1,) + (1,) * (values.ndim - 1 - position))

    near = jax.random.permutation(rng, shards_of)[block_of(target)]
    far = (block_of(target) + shards_of // 2) % shards_of
    return jnp.where((block_of(source) == near) | (block_of(source) == far), factor * values, values)


def level_of(stream_key, shape, cuts, smallest, high):
    gain = 1.0
    for position, shards_of in cuts:
        draws = jax.random.uniform(jax.random.fold_in(jax.random.fold_in(stream_key, 6), position), (shards_of,), jnp.float32, smallest / len(cuts), high / len(cuts))
        gain = gain * jnp.repeat(jnp.exp(draws), shape[position] // shards_of).reshape((-1,) + (1,) * (len(shape) - 1 - position))
    return gain


def normal_values(stream_key, dims, deviation, reach, cuts=(), dtype=jnp.bfloat16):
    drawn = deviation * jax.random.normal(stream_key, dims, jnp.float32)
    if cuts:
        drawn = drawn * level_of(stream_key, dims, cuts, -0.22, 0.18)
    return jnp.clip(drawn, -reach, reach).astype(dtype)


def bell_draw_with(stream_key, shape, scale, limit, cuts, heavy, dtype=jnp.bfloat16):
    array = scale * jax.random.normal(stream_key, shape, jnp.float32)
    if cuts:
        array = array * level_of(stream_key, shape, cuts, -0.22, 0.18)
    return jnp.clip(spiked(array, jax.random.fold_in(stream_key, 3), *heavy), -limit, limit).astype(dtype)


def setup_inputs(seed: int = 0) -> dict:
    splits = jax.random.split(jax.random.key(seed), 7)
    queries = normal_values(splits[0], (SEQUENCE_TOKENS, D), 1.0, 6.0, ((0, 32), (1, 4)))
    key_vectors = normal_values(splits[1], (SEQUENCE_TOKENS, D), 1.0, 6.0, ((0, 32), (1, 4)))
    value_vectors = normal_values(splits[2], (SEQUENCE_TOKENS, D), 1.0, 6.0, ((0, 32), (1, 4)))
    out_grad = normal_values(splits[3], (SEQUENCE_TOKENS, D), (4.0 / SEQUENCE_TOKENS ** 0.5), 0.25, ((0, 32), (1, 4)))
    log_decay = draw_log_decay(jax.random.fold_in(splits[6], 71), 0)
    inputs = bell_draw_with(splits[5], (SEQUENCE_TOKENS, D), (SEQUENCE_TOKENS ** -0.5), 0.109375, ((0, 32),), (0, 1, 32, 2.75))
    return dict(queries=queries, key_vectors=key_vectors, value_vectors=value_vectors, out_grad=out_grad, log_decay=log_decay, inputs=inputs)


def local_grads(carry_low, queries, key_vectors, value_vectors, out_grad, cumulated, totals):
    factor = DH ** -0.5
    spread = cumulated.T[:, :, None] - cumulated.T[:, None, :]
    row_index = lax.broadcasted_iota(jnp.int32, spread.shape, 1)
    column_index = lax.broadcasted_iota(jnp.int32, spread.shape, 2)
    weights = jnp.where(row_index >= column_index, jnp.exp(jnp.minimum(spread, 0.0)), 0.0)
    query_wide = queries.astype(jnp.float32)
    key_wide = key_vectors.astype(jnp.float32)
    value_wide = value_vectors.astype(jnp.float32)
    grad_wide = out_grad.astype(jnp.float32)
    carry_wide = carry_low.astype(jnp.float32)
    key_scores = (factor * jnp.einsum("thd,shd->hts", query_wide, key_wide) * weights).astype(jnp.bfloat16)
    grad_scores = (factor * jnp.einsum("thd,shd->hts", grad_wide, value_wide) * weights).astype(jnp.bfloat16)
    decayed = jnp.exp(totals[None, :] - cumulated)[:, :, None]
    key_grad = jnp.einsum("hts,thd->shd", grad_scores.astype(jnp.float32), query_wide) + decayed * jnp.einsum("she,hde->shd", value_wide, carry_wide)
    value_grad = jnp.einsum("hts,the->she", key_scores.astype(jnp.float32), grad_wide) + decayed * jnp.einsum("shd,hde->she", key_wide, carry_wide)
    return key_grad.astype(jnp.bfloat16), value_grad.astype(jnp.bfloat16)


def into_blocks(matrix):
    return matrix.reshape(matrix.shape[0] // BLOCK, BLOCK, H, DH)


def reference(queries, key_vectors, value_vectors, out_grad, log_decay, inputs):
    token_count = queries.shape[0]
    block_count = token_count // BLOCK
    cumulated = jnp.cumsum(log_decay.reshape(H, block_count, BLOCK), axis=2).transpose(1, 2, 0)
    totals = cumulated[:, -1, :]
    query_blocks = into_blocks(queries)
    grad_blocks = into_blocks(out_grad)
    weighted = (query_blocks.astype(jnp.float32) * (DH ** -0.5 * jnp.exp(cumulated))[..., None]).astype(jnp.bfloat16)

    def advance(carried, pieces):
        query_block, key_block, value_block, grad_block, cum_block, total_block, weighted_block = pieces
        key_grad, value_grad = local_grads(carried.astype(jnp.bfloat16), query_block, key_block, value_block, grad_block, cum_block, total_block)
        block_state = jnp.einsum("thd,the->hde", weighted_block.astype(jnp.float32), grad_block.astype(jnp.float32))
        return jnp.exp(total_block)[:, None, None] * carried + block_state, (key_grad, value_grad)

    start_value = jnp.zeros((H, DH, DH), jnp.float32)
    pieces = (query_blocks, into_blocks(key_vectors), into_blocks(value_vectors), grad_blocks, cumulated, totals, weighted)
    unused, gradients = lax.scan(advance, start_value, pieces, reverse=True)
    key_grad = gradients[0].reshape(token_count, H * DH)
    value_grad = gradients[1].reshape(token_count, H * DH)
    key_part = jnp.dot(inputs.T, key_grad, preferred_element_type=jnp.float32)
    value_part = jnp.dot(inputs.T, value_grad, preferred_element_type=jnp.float32)
    weight_grad = jnp.stack([key_part, value_part], axis=1).astype(jnp.bfloat16)
    return key_grad, value_grad, weight_grad
```

```python
import functools

import jax
import jax.numpy as jnp
from jax import lax
from jax.experimental import pallas as pl
from jax.experimental.pallas import tpu as pltpu
from jax.sharding import Mesh
from jax.sharding import PartitionSpec as P

DH = 256
BLOCK = 512
Z, X, Y = ("z", "x", "y")
SEQ = (Z, X, Y)
TP = ("lo", "core")
EVERY = SEQ + TP
F32 = jnp.float32
BF16 = jnp.bfloat16
SCALE = DH ** (-0.5)


def cumulate(rows):
    lane = lax.broadcasted_iota(jnp.int32, rows.shape, 1)
    step = 1
    while step < rows.shape[1]:
        rows = rows + jnp.where(lane >= step, pltpu.roll(rows, step, 1), 0.0)
        step *= 2
    return rows


def pick_row(rows, head):
    index = lax.broadcasted_iota(jnp.int32, rows.shape, 0)
    return jnp.sum(jnp.where(index == head, rows, 0.0), axis=0, keepdims=True)


def pick_column(columns, head):
    index = lax.broadcasted_iota(jnp.int32, columns.shape, 1)
    return jnp.sum(jnp.where(index == head, columns, 0.0), axis=1, keepdims=True)


def dot_tt(a, b):
    return lax.dot_general(a, b, (((0,), (0,)), ((), ())), preferred_element_type=F32)


def dot_nt(a, b):
    return lax.dot_general(a, b, (((1,), (1,)), ((), ())), preferred_element_type=F32)


def dot_nn(a, b):
    return jnp.dot(a, b, preferred_element_type=F32)


def states_kernel(heads, where_ref, q_ref, g_ref, ld_ref, state_ref, message_ref, total, passed):
    block = pl.program_id(0)
    first = where_ref[0] * heads

    @pl.when(block == 0)
    def _():
        total[...] = jnp.zeros_like(total)
        passed[...] = jnp.zeros_like(passed)

    cum = cumulate(ld_ref[...])
    columns = cum.T
    for h in range(heads):
        cols = slice(h * DH, (h + 1) * DH)
        decay = SCALE * jnp.exp(pick_column(columns, first + h))
        weighted = (q_ref[:, cols].astype(F32) * decay).astype(BF16)
        state = dot_tt(weighted, g_ref[:, cols])
        state_ref[0, h] = state
        before = passed[h, 0:1, 0:1]
        total[h] = total[h] + jnp.exp(before) * state
        last = pick_row(cum, first + h)[:, -1:]
        passed[h] = passed[h] + last

    @pl.when(block == pl.num_programs(0) - 1)
    def _():
        piece = message_ref.shape[1]
        each = DH // piece
        row = lax.broadcasted_iota(jnp.int32, (piece, 128), 0)
        for h in range(heads):
            gone = jnp.broadcast_to(passed[h, 0:1, 0:1], (piece, 128))
            high = gone.astype(BF16).astype(F32)
            middle = (gone - high).astype(BF16).astype(F32)
            low = gone - high - middle
            tail = jnp.where(row == 0, high, jnp.where(row == 1, middle, jnp.where(row == 2, low, 0.0)))
            tail = tail.astype(BF16)
            for k in range(each):
                message_ref[h * each + k, :, :DH] = total[h, k * piece : (k + 1) * piece, :].astype(BF16)
                message_ref[h * each + k, :, DH:] = tail


def block_states(place, queries, out_grad, log_decay, devices):
    rows, width = queries.shape
    heads = width // DH
    blocks = rows // BLOCK
    piece = heads * DH // devices
    return pl.pallas_call(
        functools.partial(states_kernel, heads),
        grid_spec=pltpu.PrefetchScalarGridSpec(
            num_scalar_prefetch=1,
            grid=(blocks,),
            in_specs=[
                pl.BlockSpec((BLOCK, width), lambda i, s: (i, 0)),
                pl.BlockSpec((BLOCK, width), lambda i, s: (i, 0)),
                pl.BlockSpec((log_decay.shape[0], BLOCK), lambda i, s: (0, i)),
            ],
            out_specs=[
                pl.BlockSpec((1, heads, DH, DH), lambda i, s: (i, 0, 0, 0)),
                pl.BlockSpec((devices, piece, DH + 128), lambda i, s: (0, 0, 0)),
            ],
            scratch_shapes=[pltpu.VMEM((heads, DH, DH), F32), pltpu.VMEM((heads, 8, 128), F32)],
        ),
        out_shape=[
            jax.ShapeDtypeStruct((blocks, heads, DH, DH), F32),
            jax.ShapeDtypeStruct((devices, piece, DH + 128), BF16),
        ],
        cost_estimate=pl.CostEstimate(
            flops=2 * rows * width * DH, bytes_accessed=4 * rows * width + 4 * blocks * width * DH, transcendentals=rows
        ),
        name="states",
    )(place, queries, out_grad, log_decay)


def chain_kernel(message_ref, out_ref):
    devices, piece, _ = message_ref.shape
    carried = jnp.zeros((piece, DH), F32)
    for d in reversed(range(devices)):
        out_ref[d] = carried.astype(BF16)
        logs = jnp.sum(message_ref[d, :, DH:].astype(F32), axis=0, keepdims=True)
        gamma = jnp.exp(logs)
        gamma = jnp.concatenate([gamma] * (DH // 128), axis=1)
        carried = message_ref[d, :, :DH].astype(F32) + gamma * carried


def chain(message):
    devices, piece, _ = message.shape
    return pl.pallas_call(
        chain_kernel,
        out_shape=jax.ShapeDtypeStruct((devices, piece, DH), BF16),
        cost_estimate=pl.CostEstimate(flops=4 * devices * piece * DH, bytes_accessed=4 * message.size, transcendentals=0),
        name="chain",
    )(message)


def inside_kernel(heads, where_ref, q_ref, k_ref, v_ref, g_ref, ld_ref, ik_ref, iv_ref):
    first = where_ref[0] * heads
    cum = cumulate(ld_ref[...])
    columns = cum.T
    row = lax.broadcasted_iota(jnp.int32, (BLOCK, BLOCK), 0)
    column = lax.broadcasted_iota(jnp.int32, (BLOCK, BLOCK), 1)
    seen = row >= column
    for h in range(heads):
        cols = slice(h * DH, (h + 1) * DH)
        spread = pick_column(columns, first + h) - pick_row(cum, first + h)
        weights = jnp.where(seen, SCALE * jnp.exp(jnp.minimum(spread, 0.0)), 0.0)
        q, k, v, g = (ref[:, cols] for ref in (q_ref, k_ref, v_ref, g_ref))
        key_scores = (dot_nt(q, k) * weights).astype(BF16)
        grad_scores = (dot_nt(g, v) * weights).astype(BF16)
        ik_ref[:, cols] = dot_tt(grad_scores, q)
        iv_ref[:, cols] = dot_tt(key_scores, g)


def inside(place, queries, keys, values, out_grad, log_decay):
    rows, width = queries.shape
    heads = width // DH
    tokens = pl.BlockSpec((BLOCK, width), lambda i, s: (i, 0))
    return pl.pallas_call(
        functools.partial(inside_kernel, heads),
        grid_spec=pltpu.PrefetchScalarGridSpec(
            num_scalar_prefetch=1,
            grid=(rows // BLOCK,),
            in_specs=[tokens] * 4 + [pl.BlockSpec((log_decay.shape[0], BLOCK), lambda i, s: (0, i))],
            out_specs=[tokens] * 2,
        ),
        out_shape=[jax.ShapeDtypeStruct((rows, width), F32)] * 2,
        cost_estimate=pl.CostEstimate(
            flops=8 * rows * width * BLOCK, bytes_accessed=16 * rows * width, transcendentals=rows * BLOCK * heads
        ),
        name="inside",
    )(place, queries, keys, values, out_grad, log_decay)


def finish_kernel(heads, where_ref, c_ref, state_ref, k_ref, v_ref, ld_ref, ik_ref, iv_ref, kg_ref, vg_ref, carry):
    first = where_ref[0] * heads

    @pl.when(pl.program_id(0) == 0)
    def _():
        carry[...] = c_ref[...].astype(F32)

    cum = cumulate(ld_ref[...])
    columns = cum.T
    for h in range(heads):
        cols = slice(h * DH, (h + 1) * DH)
        last = pick_row(cum, first + h)[:, -1:]
        decayed = jnp.exp(last - pick_column(columns, first + h))
        low = carry[h].astype(BF16)
        kg_ref[:, cols] = (ik_ref[:, cols] + decayed * dot_nt(v_ref[:, cols], low)).astype(BF16)
        vg_ref[:, cols] = (iv_ref[:, cols] + decayed * dot_nn(k_ref[:, cols], low)).astype(BF16)
        carry[h] = jnp.exp(last) * carry[h] + state_ref[0, h]


def finish(place, carried, states, keys, values, log_decay, ik, iv):
    rows, width = keys.shape
    heads = width // DH
    blocks = rows // BLOCK
    tokens = pl.BlockSpec((BLOCK, width), lambda i, s: (blocks - 1 - i, 0))
    return pl.pallas_call(
        functools.partial(finish_kernel, heads),
        grid_spec=pltpu.PrefetchScalarGridSpec(
            num_scalar_prefetch=1,
            grid=(blocks,),
            in_specs=[
                pl.BlockSpec((heads, DH, DH), lambda i, s: (0, 0, 0)),
                pl.BlockSpec((1, heads, DH, DH), lambda i, s: (blocks - 1 - i, 0, 0, 0)),
                tokens,
                tokens,
                pl.BlockSpec((log_decay.shape[0], BLOCK), lambda i, s: (0, blocks - 1 - i)),
                tokens,
                tokens,
            ],
            out_specs=[tokens] * 2,
            scratch_shapes=[pltpu.VMEM((heads, DH, DH), F32)],
        ),
        out_shape=[jax.ShapeDtypeStruct((rows, width), BF16)] * 2,
        cost_estimate=pl.CostEstimate(
            flops=4 * rows * width * DH, bytes_accessed=16 * rows * width, transcendentals=rows * heads
        ),
        name="finish",
    )(place, carried, states, keys, values, log_decay, ik, iv)


def weight_kernel(where_ref, a_ref, b_ref, c_ref, d_ref, grad_ref, out_ref):
    part = a_ref.shape[1]
    grad = grad_ref[...]
    for i, ref in enumerate((a_ref, b_ref, c_ref, d_ref)):
        out_ref[0, i * part : (i + 1) * part, :] = dot_tt(ref[...], grad).astype(BF16)


def weight_part(place, inputs, grad):
    tokens, rows = inputs.shape
    width = grad.shape[1]
    part = rows // 16

    def columns(i):
        return pl.BlockSpec((tokens, part), lambda j, s: (0, jnp.where(s[1] == 0, 4 * j + i, 4 * i + j)))

    return pl.pallas_call(
        weight_kernel,
        grid_spec=pltpu.PrefetchScalarGridSpec(
            num_scalar_prefetch=1,
            grid=(4,),
            in_specs=[columns(i) for i in range(4)] + [pl.BlockSpec((tokens, width), lambda j, s: (0, 0))],
            out_specs=pl.BlockSpec((1, rows // 4, width), lambda j, s: (j, 0, 0)),
        ),
        out_shape=jax.ShapeDtypeStruct((4, rows // 4, width), BF16),
        cost_estimate=pl.CostEstimate(
            flops=2 * tokens * rows * width, bytes_accessed=2 * tokens * (rows + width) + 2 * rows * width, transcendentals=0
        ),
        name="weights",
    )(place, inputs, inputs, inputs, inputs, grad)


def groups_of(first, second):
    def index(z, x, y, lo, core):
        return (((z * 4 + x) * 2 + y) * 2 + lo) * 2 + core

    out = []
    for core, axis in ((0, first), (1, second)):
        for y in range(2):
            for lo in range(2):
                for other in range(4):
                    out.append(
                        [
                            index(k, other, y, lo, core) if axis == Z else index(other, k, y, lo, core)
                            for k in range(4)
                        ]
                    )
    return out


def exchange(pieces, groups):
    return lax.all_to_all(pieces, EVERY, 0, 0, axis_index_groups=groups, tiled=True)


def summed(pieces):
    return pieces.astype(F32).sum(axis=0).astype(BF16)


def sum_at_owner(pieces):
    width = pieces.shape[-1]
    mine = summed(exchange(pieces, groups_of(Z, X)))
    mine = summed(exchange(mine.reshape(4, -1, width), groups_of(X, Z)))
    return summed(lax.all_to_all(mine.reshape(2, -1, width), Y, 0, 0, tiled=True))


def shards(queries, keys, values, out_grad, log_decay, inputs):
    devices = lax.axis_size(SEQ)
    place = jnp.stack([lax.axis_index(TP), lax.axis_index("core")]).astype(jnp.int32)
    states, message = block_states(place, queries, out_grad, log_decay, devices)
    arrived = lax.all_to_all(message, SEQ, 0, 0, tiled=True)
    ik, iv = inside(place, queries, keys, values, out_grad, log_decay)
    carried = lax.all_to_all(chain(arrived), SEQ, 0, 0, tiled=True)
    carried = carried.reshape(-1, DH, DH)
    key_grad, value_grad = finish(place, carried, states, keys, values, log_decay, ik, iv)
    sums = [sum_at_owner(weight_part(place, inputs, grad)) for grad in (key_grad, value_grad)]
    return (key_grad, value_grad, jnp.stack(sums, axis=1))


def solution(mesh):
    split = Mesh(mesh.devices.reshape(4, 4, 2, 2, 2), EVERY)
    placed = (P(SEQ, TP),) * 4 + (P(None, SEQ), P(SEQ, None))
    return jax.shard_map(
        shards,
        mesh=split,
        in_specs=placed,
        out_specs=(P(SEQ, TP), P(SEQ, TP), P(SEQ, None, TP)),
        check_vma=False,
    )
```

```python
import functools

import jax
import jax.numpy as jnp
from jax import lax
from jax.experimental import pallas as pl
from jax.experimental.pallas import tpu as pltpu
from jax.sharding import Mesh
from jax.sharding import PartitionSpec as P

DH = 256
BLOCK = 512
SEQ = ("z", "x", "y")
TP = ("lo", "core")
EVERY = SEQ + TP
F32 = jnp.float32
BF16 = jnp.bfloat16
SCALE = DH ** (-0.5)


def cumulate(rows):
    lane = lax.broadcasted_iota(jnp.int32, rows.shape, 1)
    step = 1
    while step < rows.shape[1]:
        rows = rows + jnp.where(lane >= step, pltpu.roll(rows, step, 1), 0.0)
        step *= 2
    return rows


def own_rows(rows, first, heads):
    index = lax.broadcasted_iota(jnp.int32, rows.shape, 0)
    picked = [jnp.sum(jnp.where(index == first + h, rows, 0.0), axis=0, keepdims=True) for h in range(heads)]
    out = jnp.zeros_like(rows)
    for h in range(heads):
        out = jnp.where(index == h, picked[h], out)
    return out


def dot_tt(a, b):
    return lax.dot_general(a, b, (((0,), (0,)), ((), ())), preferred_element_type=F32)


def dot_nt(a, b):
    return lax.dot_general(a, b, (((1,), (1,)), ((), ())), preferred_element_type=F32)


def dot_nn(a, b):
    return jnp.dot(a, b, preferred_element_type=F32)


def states_kernel(heads, where_ref, q_ref, g_ref, ld_ref, state_ref, message_ref, total, passed):
    block = pl.program_id(0)

    @pl.when(block == 0)
    def _():
        total[...] = jnp.zeros_like(total)
        passed[...] = jnp.zeros_like(passed)

    cum = cumulate(own_rows(ld_ref[...], where_ref[0] * heads, heads))
    decay = (SCALE * jnp.exp(cum)).T
    for h in range(heads):
        cols = slice(h * DH, (h + 1) * DH)
        weighted = (q_ref[:, cols].astype(F32) * decay[:, h : h + 1]).astype(BF16)
        state = dot_tt(weighted, g_ref[:, cols])
        state_ref[0, h] = state
        total[h] = total[h] + jnp.exp(passed[h : h + 1, 0:1]) * state
    passed[...] = passed[...] + cum[:, BLOCK - 1 : BLOCK]

    @pl.when(block == pl.num_programs(0) - 1)
    def _():
        piece = message_ref.shape[1]
        each = DH // piece
        row = lax.broadcasted_iota(jnp.int32, (piece, 128), 0)
        for h in range(heads):
            gone = jnp.broadcast_to(passed[h : h + 1, :], (piece, 128))
            high = gone.astype(BF16).astype(F32)
            middle = (gone - high).astype(BF16).astype(F32)
            low = gone - high - middle
            tail = jnp.where(row == 0, high, jnp.where(row == 1, middle, jnp.where(row == 2, low, 0.0)))
            tail = tail.astype(BF16)
            for k in range(each):
                message_ref[h * each + k, :, :DH] = total[h, k * piece : (k + 1) * piece, :].astype(BF16)
                message_ref[h * each + k, :, DH:] = tail


def block_states(place, queries, out_grad, log_decay, devices):
    rows, width = queries.shape
    heads = width // DH
    blocks = rows // BLOCK
    piece = heads * DH // devices
    return pl.pallas_call(
        functools.partial(states_kernel, heads),
        grid_spec=pltpu.PrefetchScalarGridSpec(
            num_scalar_prefetch=1,
            grid=(blocks,),
            in_specs=[
                pl.BlockSpec((BLOCK, width), lambda i, s: (i, 0)),
                pl.BlockSpec((BLOCK, width), lambda i, s: (i, 0)),
                pl.BlockSpec((log_decay.shape[0], BLOCK), lambda i, s: (0, i)),
            ],
            out_specs=[
                pl.BlockSpec((1, heads, DH, DH), lambda i, s: (i, 0, 0, 0)),
                pl.BlockSpec((devices, piece, DH + 128), lambda i, s: (0, 0, 0)),
            ],
            scratch_shapes=[pltpu.VMEM((heads, DH, DH), F32), pltpu.VMEM((log_decay.shape[0], 128), F32)],
        ),
        out_shape=[
            jax.ShapeDtypeStruct((blocks, heads, DH, DH), F32),
            jax.ShapeDtypeStruct((devices, piece, DH + 128), BF16),
        ],
        cost_estimate=pl.CostEstimate(
            flops=2 * rows * width * DH, bytes_accessed=4 * rows * width + 4 * blocks * width * DH, transcendentals=rows
        ),
        name="states",
    )(place, queries, out_grad, log_decay)


def chain_kernel(message_ref, out_ref):
    devices, piece, _ = message_ref.shape
    carried = jnp.zeros((piece, DH), F32)
    for d in reversed(range(devices)):
        out_ref[d] = carried.astype(BF16)
        logs = jnp.sum(message_ref[d, :, DH:].astype(F32), axis=0, keepdims=True)
        gamma = jnp.exp(logs)
        gamma = jnp.concatenate([gamma] * (DH // 128), axis=1)
        carried = message_ref[d, :, :DH].astype(F32) + gamma * carried


def chain(message):
    devices, piece, _ = message.shape
    return pl.pallas_call(
        chain_kernel,
        out_shape=jax.ShapeDtypeStruct((devices, piece, DH), BF16),
        cost_estimate=pl.CostEstimate(flops=4 * devices * piece * DH, bytes_accessed=4 * message.size, transcendentals=0),
        name="chain",
    )(message)


def inside_kernel(heads, head, where_ref, q_ref, k_ref, v_ref, g_ref, ld_ref, ik_ref, iv_ref):
    cum = cumulate(own_rows(ld_ref[...], where_ref[0] * heads, heads))
    columns = cum.T
    half = BLOCK // 2
    row = lax.broadcasted_iota(jnp.int32, (half, half), 0)
    column = lax.broadcasted_iota(jnp.int32, (half, half), 1)
    seen = row >= column
    for j in range(2):
        sources = slice(j * half, (j + 1) * half)
        k, v = (k_ref[sources, :], v_ref[sources, :])
        key_part = value_part = None
        for i in range(j, 2):
            targets = slice(i * half, (i + 1) * half)
            q, g = (q_ref[targets, :], g_ref[targets, :])
            spread = columns[targets, head : head + 1] - cum[head : head + 1, sources]
            weights = SCALE * jnp.exp(jnp.minimum(spread, 0.0))
            if i == j:
                weights = jnp.where(seen, weights, 0.0)
            key_scores = (dot_nt(q, k) * weights).astype(BF16)
            grad_scores = (dot_nt(g, v) * weights).astype(BF16)
            to_key, to_value = (dot_tt(grad_scores, q), dot_tt(key_scores, g))
            key_part = to_key if key_part is None else key_part + to_key
            value_part = to_value if value_part is None else value_part + to_value
        ik_ref[sources, :] = key_part
        iv_ref[sources, :] = value_part


def inside(place, head, queries, keys, values, out_grad, log_decay):
    rows, width = queries.shape
    heads = width // DH
    tokens = pl.BlockSpec((BLOCK, DH), lambda i, s: (i, head))
    return pl.pallas_call(
        functools.partial(inside_kernel, heads, head),
        grid_spec=pltpu.PrefetchScalarGridSpec(
            num_scalar_prefetch=1,
            grid=(rows // BLOCK,),
            in_specs=[tokens] * 4 + [pl.BlockSpec((log_decay.shape[0], BLOCK), lambda i, s: (0, i))],
            out_specs=[pl.BlockSpec((BLOCK, DH), lambda i, s: (i, 0))] * 2,
        ),
        out_shape=[jax.ShapeDtypeStruct((rows, DH), F32)] * 2,
        cost_estimate=pl.CostEstimate(
            flops=8 * rows * DH * BLOCK, bytes_accessed=16 * rows * DH, transcendentals=rows * BLOCK
        ),
        name=f"inside{head}",
    )(place, queries, keys, values, out_grad, log_decay)


def finish_kernel(heads, blocks, where_ref, c_ref, state_ref, k_ref, v_ref, ld_ref, *refs):
    inner = refs[: 2 * heads]
    x_ref, kg_ref, vg_ref, out_ref, carry, grads = refs[2 * heads :]
    step = pl.program_id(0)
    width = heads * DH

    @pl.when(step == 0)
    def _():
        carry[...] = c_ref[...].astype(F32)

    @pl.when(step < blocks)
    def _():
        cum = cumulate(own_rows(ld_ref[...], where_ref[0] * heads, heads))
        last = cum[:, BLOCK - 1 : BLOCK]
        decayed = jnp.exp(last - cum).T
        rows = pl.ds(pl.multiple_of((blocks - 1 - step) * BLOCK, BLOCK), BLOCK)
        for h in range(heads):
            cols = slice(h * DH, (h + 1) * DH)
            low = carry[h].astype(BF16)
            over = decayed[:, h : h + 1]
            key_grad = (inner[2 * h][...] + over * dot_nt(v_ref[:, cols], low)).astype(BF16)
            value_grad = (inner[2 * h + 1][...] + over * dot_nn(k_ref[:, cols], low)).astype(BF16)
            kg_ref[:, cols] = key_grad
            vg_ref[:, cols] = value_grad
            grads[rows, cols] = key_grad
            grads[rows, width + h * DH : width + (h + 1) * DH] = value_grad
            carry[h] = jnp.exp(last[h : h + 1, :]) * carry[h] + state_ref[0, h]

    @pl.when(step >= blocks)
    def _():
        devices, share, lanes = out_ref.shape
        strips = 2 * width // lanes
        share = share // strips
        for part in range(2):
            sums = dot_tt(x_ref[...], grads[:, part * width : (part + 1) * width]).astype(BF16)
            for d in range(devices):
                for c in range(width // lanes):
                    at = (part * (width // lanes) + c) * share
                    out_ref[d, at : at + share, :] = sums[d * share : (d + 1) * share, c * lanes : (c + 1) * lanes]


def finish(place, carried, states, keys, values, log_decay, inner, inputs, devices):
    rows, width = keys.shape
    heads = width // DH
    blocks = rows // BLOCK
    steps = 4
    wide = inputs.shape[1]
    share = wide // devices

    def back(i):
        return jnp.maximum(blocks - 1 - i, 0)

    def later(i):
        return jnp.maximum(i - blocks, 0)

    tokens = pl.BlockSpec((BLOCK, width), lambda i, s: (back(i), 0))
    return pl.pallas_call(
        functools.partial(finish_kernel, heads, blocks),
        grid_spec=pltpu.PrefetchScalarGridSpec(
            num_scalar_prefetch=1,
            grid=(blocks + steps,),
            in_specs=[
                pl.BlockSpec((heads, DH, DH), lambda i, s: (0, 0, 0)),
                pl.BlockSpec((1, heads, DH, DH), lambda i, s: (back(i), 0, 0, 0)),
                tokens,
                tokens,
                pl.BlockSpec((log_decay.shape[0], BLOCK), lambda i, s: (0, back(i))),
            ]
            + [pl.BlockSpec((BLOCK, DH), lambda i, s: (back(i), 0))] * (2 * heads)
            + [pl.BlockSpec((rows, wide // steps), lambda i, s: (0, later(i)))],
            out_specs=[
                tokens,
                tokens,
                pl.BlockSpec((devices // steps, 2 * share * width // 128, 128), lambda i, s: (later(i), 0, 0)),
            ],
            scratch_shapes=[pltpu.VMEM((heads, DH, DH), F32), pltpu.VMEM((rows, 2 * width), BF16)],
        ),
        out_shape=[jax.ShapeDtypeStruct((rows, width), BF16)] * 2
        + [pltpu.VMEM((devices, 2 * share * width // 128, 128), BF16)],
        cost_estimate=pl.CostEstimate(
            flops=4 * rows * width * (DH + wide), bytes_accessed=16 * rows * width, transcendentals=rows * heads
        ),
        compiler_params=pltpu.CompilerParams(vmem_limit_bytes=48 << 20),
        name="finish",
    )(place, carried, states, keys, values, log_decay, *inner, inputs)


def gather_kernel(parts_ref, out_ref):
    devices, rows, lanes = parts_ref.shape
    share, _, width = out_ref.shape
    strips = width // lanes
    step = 32
    for start in range(0, rows, step):
        total = parts_ref[0, start : start + step, :].astype(F32)
        for d in range(1, devices):
            total = total + parts_ref[d, start : start + step, :].astype(F32)
        part, strip = divmod(start // share, strips)
        at = start % share
        out_ref[at : at + step, part, strip * lanes : (strip + 1) * lanes] = total.astype(BF16)


def gathered(parts, width):
    rows = parts.shape[1] * parts.shape[2] // width
    return pl.pallas_call(
        gather_kernel,
        in_specs=[pl.BlockSpec(memory_space=pltpu.VMEM)],
        out_shape=jax.ShapeDtypeStruct((rows // 2, 2, width), BF16),
        cost_estimate=pl.CostEstimate(flops=parts.size, bytes_accessed=2 * parts.size, transcendentals=0),
        compiler_params=pltpu.CompilerParams(vmem_limit_bytes=12 << 20),
        name="gathered",
    )(parts)


def shards(queries, keys, values, out_grad, log_decay, inputs):
    devices = lax.axis_size(SEQ)
    width = queries.shape[1]
    place = lax.axis_index(TP).astype(jnp.int32).reshape(1)
    states, message = block_states(place, queries, out_grad, log_decay, devices)
    tokens = (queries, keys, values, out_grad, log_decay)
    arrived = lax.all_to_all(message, SEQ, 0, 0, tiled=True)
    inner = list(inside(place, 0, *tokens))
    arrived, place, *inner = lax.optimization_barrier((arrived, place, *inner))
    carried = lax.all_to_all(chain(arrived), SEQ, 0, 0, tiled=True)
    inner += inside(place, 1, *tokens)
    key_grad, value_grad, parts = finish(
        place, carried.reshape(-1, DH, DH), states, keys, values, log_decay, inner, inputs, devices
    )
    parts = lax.all_to_all(parts, SEQ, 0, 0, tiled=True)
    return (key_grad, value_grad, gathered(parts, width))


def solution(mesh):
    split = Mesh(mesh.devices.reshape(4, 4, 2, 2, 2), EVERY)
    placed = (P(SEQ, TP),) * 4 + (P(None, SEQ), P(SEQ, None))
    return jax.shard_map(
        shards,
        mesh=split,
        in_specs=placed,
        out_specs=(P(SEQ, TP), P(SEQ, TP), P(SEQ, None, TP)),
        check_vma=False,
    )
```

```python
import functools
import itertools

import jax
import jax.numpy as jnp
from jax import lax
from jax.experimental import pallas as pl
from jax.experimental.pallas import tpu as pltpu
from jax.sharding import Mesh
from jax.sharding import PartitionSpec as P

DH = 256
BLOCK = 512
SEQ = ("z", "x", "y")
TP = ("lo", "core")
EVERY = SEQ + TP
F32 = jnp.float32
BF16 = jnp.bfloat16
SCALE = DH ** (-0.5)


def cumulate(rows):
    lane = lax.rem(lax.broadcasted_iota(jnp.int32, rows.shape, 1), BLOCK)
    step = 1
    while step < BLOCK:
        rows = rows + jnp.where(lane >= step, pltpu.roll(rows, step, 1), 0.0)
        step *= 2
    return rows


def own_rows(rows, first, heads):
    index = lax.broadcasted_iota(jnp.int32, rows.shape, 0)
    picked = [jnp.sum(jnp.where(index == first + h, rows, 0.0), axis=0, keepdims=True) for h in range(heads)]
    out = jnp.zeros_like(rows)
    for h in range(heads):
        out = jnp.where(index == h, picked[h], out)
    return out


def dot_tt(a, b):
    return lax.dot_general(a, b, (((0,), (0,)), ((), ())), preferred_element_type=F32)


def dot_nt(a, b):
    return lax.dot_general(a, b, (((1,), (1,)), ((), ())), preferred_element_type=F32)


def dot_nn(a, b):
    return jnp.dot(a, b, preferred_element_type=F32)


def states_kernel(heads, where_ref, q_ref, g_ref, ld_ref, state_ref, message_ref, total, passed):
    block = pl.program_id(0)

    @pl.when(block == 0)
    def _():
        total[...] = jnp.zeros_like(total)
        passed[...] = jnp.zeros_like(passed)

    cum = cumulate(own_rows(ld_ref[...], where_ref[0] * heads, heads))
    decay = (SCALE * jnp.exp(cum)).T
    before = passed[:, 0:1]
    sums = [total[h] for h in range(heads)]
    for c in range(state_ref.shape[0]):
        rows = slice(c * BLOCK, (c + 1) * BLOCK)
        kept = jnp.exp(before)
        for h in range(heads):
            cols = slice(h * DH, (h + 1) * DH)
            weighted = (q_ref[rows, cols].astype(F32) * decay[rows, h : h + 1]).astype(BF16)
            state = dot_tt(weighted, g_ref[rows, cols])
            state_ref[c, h] = state
            sums[h] = sums[h] + kept[h : h + 1, :] * state
        before = before + cum[:, (c + 1) * BLOCK - 1 : (c + 1) * BLOCK]
    for h in range(heads):
        total[h] = sums[h]
    passed[...] = jnp.broadcast_to(before, passed.shape)

    @pl.when(block == pl.num_programs(0) - 1)
    def _():
        piece = message_ref.shape[1]
        each = DH // piece
        row = lax.broadcasted_iota(jnp.int32, (piece, 128), 0)
        for h in range(heads):
            gone = jnp.broadcast_to(passed[h : h + 1, :], (piece, 128))
            high = gone.astype(BF16).astype(F32)
            middle = (gone - high).astype(BF16).astype(F32)
            low = gone - high - middle
            tail = jnp.where(row == 0, high, jnp.where(row == 1, middle, jnp.where(row == 2, low, 0.0)))
            tail = tail.astype(BF16)
            for k in range(each):
                message_ref[h * each + k, :, :DH] = total[h, k * piece : (k + 1) * piece, :].astype(BF16)
                message_ref[h * each + k, :, DH:] = tail


def block_states(place, queries, out_grad, log_decay, devices):
    rows, width = queries.shape
    heads = width // DH
    blocks = rows // BLOCK
    piece = heads * DH // devices
    per = 2
    return pl.pallas_call(
        functools.partial(states_kernel, heads),
        grid_spec=pltpu.PrefetchScalarGridSpec(
            num_scalar_prefetch=1,
            grid=(blocks // per,),
            in_specs=[
                pl.BlockSpec((per * BLOCK, width), lambda i, s: (i, 0)),
                pl.BlockSpec((per * BLOCK, width), lambda i, s: (i, 0)),
                pl.BlockSpec((log_decay.shape[0], per * BLOCK), lambda i, s: (0, i)),
            ],
            out_specs=[
                pl.BlockSpec((per, heads, DH, DH), lambda i, s: (i, 0, 0, 0)),
                pl.BlockSpec((devices, piece, DH + 128), lambda i, s: (0, 0, 0)),
            ],
            scratch_shapes=[pltpu.VMEM((heads, DH, DH), F32), pltpu.VMEM((log_decay.shape[0], 128), F32)],
        ),
        out_shape=[
            jax.ShapeDtypeStruct((blocks, heads, DH, DH), F32),
            jax.ShapeDtypeStruct((devices, piece, DH + 128), BF16),
        ],
        cost_estimate=pl.CostEstimate(
            flops=2 * rows * width * DH, bytes_accessed=4 * rows * width + 4 * blocks * width * DH, transcendentals=rows
        ),
        name="states",
    )(place, queries, out_grad, log_decay)


def chain_kernel(message_ref, out_ref):
    devices, piece, _ = message_ref.shape
    carried = jnp.zeros((piece, DH), F32)
    for d in reversed(range(devices)):
        out_ref[d] = carried.astype(BF16)
        logs = jnp.sum(message_ref[d, :, DH:].astype(F32), axis=0, keepdims=True)
        gamma = jnp.exp(logs)
        gamma = jnp.concatenate([gamma] * (DH // 128), axis=1)
        carried = message_ref[d, :, :DH].astype(F32) + gamma * carried


def chain(message):
    devices, piece, _ = message.shape
    return pl.pallas_call(
        chain_kernel,
        out_shape=jax.ShapeDtypeStruct((devices, piece, DH), BF16),
        cost_estimate=pl.CostEstimate(flops=4 * devices * piece * DH, bytes_accessed=4 * message.size, transcendentals=0),
        compiler_params=pltpu.CompilerParams(vmem_limit_bytes=8 << 20),
        name="chain",
    )(message)


def inside_kernel(heads, head, where_ref, q_ref, k_ref, v_ref, g_ref, ld_ref, ik_ref, iv_ref):
    cum = cumulate(own_rows(ld_ref[...], where_ref[0] * heads, heads))
    columns = cum.T
    half = BLOCK // 2
    row = lax.broadcasted_iota(jnp.int32, (half, half), 0)
    column = lax.broadcasted_iota(jnp.int32, (half, half), 1)
    seen = row >= column
    for j in range(2):
        sources = slice(j * half, (j + 1) * half)
        k, v = (k_ref[sources, :], v_ref[sources, :])
        key_part = value_part = None
        for i in range(j, 2):
            targets = slice(i * half, (i + 1) * half)
            q, g = (q_ref[targets, :], g_ref[targets, :])
            spread = columns[targets, head : head + 1] - cum[head : head + 1, sources]
            weights = SCALE * jnp.exp(jnp.minimum(spread, 0.0))
            if i == j:
                weights = jnp.where(seen, weights, 0.0)
            key_scores = (dot_nt(q, k) * weights).astype(BF16)
            grad_scores = (dot_nt(g, v) * weights).astype(BF16)
            to_key, to_value = (dot_tt(grad_scores, q), dot_tt(key_scores, g))
            key_part = to_key if key_part is None else key_part + to_key
            value_part = to_value if value_part is None else value_part + to_value
        ik_ref[sources, :] = key_part.astype(BF16)
        iv_ref[sources, :] = value_part.astype(BF16)


def inside(place, head, queries, keys, values, out_grad, log_decay):
    rows, width = queries.shape
    heads = width // DH
    tokens = pl.BlockSpec((BLOCK, DH), lambda i, s: (i, head))
    return pl.pallas_call(
        functools.partial(inside_kernel, heads, head),
        grid_spec=pltpu.PrefetchScalarGridSpec(
            num_scalar_prefetch=1,
            grid=(rows // BLOCK,),
            in_specs=[tokens] * 4 + [pl.BlockSpec((log_decay.shape[0], BLOCK), lambda i, s: (0, i))],
            out_specs=[pl.BlockSpec((BLOCK, DH), lambda i, s: (i, 0))] * 2,
        ),
        out_shape=[jax.ShapeDtypeStruct((rows, DH), BF16)] * 2,
        cost_estimate=pl.CostEstimate(
            flops=8 * rows * DH * BLOCK, bytes_accessed=12 * rows * DH, transcendentals=rows * BLOCK
        ),
        name=f"inside{head}",
    )(place, queries, keys, values, out_grad, log_decay)


def finish_kernel(heads, blocks, where_ref, c_ref, state_ref, k_ref, v_ref, ld_ref, *refs):
    inner = refs[: 2 * heads]
    x_ref, kg_ref, vg_ref, out_ref, carry, grads = refs[2 * heads :]
    step = pl.program_id(0)
    width = heads * DH

    @pl.when(step == 0)
    def _():
        carry[...] = c_ref[...].astype(F32)

    @pl.when(step < blocks)
    def _():
        cum = cumulate(own_rows(ld_ref[...], where_ref[0] * heads, heads))
        last = cum[:, BLOCK - 1 : BLOCK]
        decayed = jnp.exp(last - cum).T
        rows = pl.ds(pl.multiple_of((blocks - 1 - step) * BLOCK, BLOCK), BLOCK)
        for h in range(heads):
            cols = slice(h * DH, (h + 1) * DH)
            low = carry[h].astype(BF16)
            over = decayed[:, h : h + 1]
            key_grad = (inner[2 * h][...].astype(F32) + over * dot_nt(v_ref[:, cols], low)).astype(BF16)
            value_grad = (inner[2 * h + 1][...].astype(F32) + over * dot_nn(k_ref[:, cols], low)).astype(BF16)
            kg_ref[:, cols] = key_grad
            vg_ref[:, cols] = value_grad
            grads[rows, cols] = key_grad
            grads[rows, width + h * DH : width + (h + 1) * DH] = value_grad
            carry[h] = jnp.exp(last[h : h + 1, :]) * carry[h] + state_ref[0, h]

    @pl.when(step >= blocks)
    def _():
        outer = step - blocks
        share = out_ref.shape[2] // 2
        for part in range(2):
            sums = dot_tt(x_ref[...], grads[:, part * width : (part + 1) * width]).astype(BF16)
            for inner_axis in range(4):
                piece = jnp.where(lax.rem(where_ref[0], 2) == 0, outer, inner_axis)
                slot = jnp.where(lax.rem(where_ref[0], 2) == 0, inner_axis, outer)
                for y in range(2):
                    at = (2 * inner_axis + y) * share
                    out_ref[piece, 2 * slot + y, part * share : (part + 1) * share, :] = sums[at : at + share, :]


def finish(place, carried, states, keys, values, log_decay, inner, inputs, devices):
    rows, width = keys.shape
    heads = width // DH
    blocks = rows // BLOCK
    steps = 4
    wide = inputs.shape[1]
    share = wide // devices

    def back(i):
        return jnp.maximum(blocks - 1 - i, 0)

    def later(i):
        return jnp.maximum(i - blocks, 0)

    tokens = pl.BlockSpec((BLOCK, width), lambda i, s: (back(i), 0))
    return pl.pallas_call(
        functools.partial(finish_kernel, heads, blocks),
        grid_spec=pltpu.PrefetchScalarGridSpec(
            num_scalar_prefetch=1,
            grid=(blocks + steps,),
            in_specs=[
                pl.BlockSpec((heads, DH, DH), lambda i, s: (0, 0, 0)),
                pl.BlockSpec((1, heads, DH, DH), lambda i, s: (back(i), 0, 0, 0)),
                tokens,
                tokens,
                pl.BlockSpec((log_decay.shape[0], BLOCK), lambda i, s: (0, back(i))),
            ]
            + [pl.BlockSpec((BLOCK, DH), lambda i, s: (back(i), 0))] * (2 * heads)
            + [pl.BlockSpec((rows, wide // steps), lambda i, s: (0, later(i)))],
            out_specs=[
                tokens,
                tokens,
                pl.BlockSpec((4, devices // 4, 2 * share, width), lambda i, s: (0, 0, 0, 0)),
            ],
            scratch_shapes=[pltpu.VMEM((heads, DH, DH), F32), pltpu.VMEM((rows, 2 * width), BF16)],
        ),
        out_shape=[jax.ShapeDtypeStruct((rows, width), BF16)] * 2
        + [pltpu.VMEM((4, devices // 4, 2 * share, width), BF16)],
        cost_estimate=pl.CostEstimate(
            flops=4 * rows * width * (DH + wide), bytes_accessed=16 * rows * width, transcendentals=rows * heads
        ),
        compiler_params=pltpu.CompilerParams(vmem_limit_bytes=48 << 20),
        name="finish",
    )(place, carried, states, keys, values, log_decay, *inner, inputs)


def near_kernel(parts_ref, out_ref):
    rows = 32
    for slot in range(out_ref.shape[0]):
        for at in range(0, out_ref.shape[1], rows):
            total = parts_ref[0, slot, at : at + rows, :].astype(F32)
            for p in range(1, parts_ref.shape[0]):
                total = total + parts_ref[p, slot, at : at + rows, :].astype(F32)
            out_ref[slot, at : at + rows, :] = total.astype(BF16)


def far_kernel(parts_ref, out_ref):
    rows = 16
    share = out_ref.shape[0]
    for start in range(0, parts_ref.shape[1], rows):
        total = parts_ref[0, start : start + rows, :].astype(F32)
        for p in range(1, parts_ref.shape[0]):
            total = total + parts_ref[p, start : start + rows, :].astype(F32)
        at = start % share
        out_ref[at : at + rows, start // share, :] = total.astype(BF16)


def summed(body, parts, shape, name):
    return pl.pallas_call(
        body,
        in_specs=[pl.BlockSpec(memory_space=pltpu.VMEM)],
        out_shape=shape,
        cost_estimate=pl.CostEstimate(flops=parts.size, bytes_accessed=2 * parts.size, transcendentals=0),
        compiler_params=pltpu.CompilerParams(vmem_limit_bytes=12 << 20),
        name=name,
    )(parts)


def groups_of(*axes_of_core):
    sizes = dict(zip(EVERY, (4, 4, 2, 2, 2)))
    out = []
    for core, axes in enumerate(axes_of_core):
        rest = [axis for axis in SEQ + ("lo",) if axis not in axes]
        for fixed in itertools.product(*(range(sizes[axis]) for axis in rest)):
            group = []
            for varied in itertools.product(*(range(sizes[axis]) for axis in axes)):
                spot = dict(zip(rest, fixed)) | dict(zip(axes, varied)) | {"core": core}
                index = 0
                for axis in EVERY:
                    index = index * sizes[axis] + spot[axis]
                group.append(index)
            out.append(group)
    return out


def exchanged(pieces, *axes_of_core):
    return lax.all_to_all(pieces, EVERY, 0, 0, axis_index_groups=groups_of(*axes_of_core), tiled=True)


def shards(queries, keys, values, out_grad, log_decay, inputs):
    devices = lax.axis_size(SEQ)
    width = queries.shape[1]
    place = lax.axis_index(TP).astype(jnp.int32).reshape(1)
    states, message = block_states(place, queries, out_grad, log_decay, devices)
    tokens = (queries, keys, values, out_grad, log_decay)
    arrived = lax.all_to_all(message, SEQ, 0, 0, tiled=True)
    inner = list(inside(place, 0, *tokens))
    arrived, place, *inner = lax.optimization_barrier((arrived, place, *inner))
    carried = lax.all_to_all(chain(arrived), SEQ, 0, 0, tiled=True)
    inner += inside(place, 1, *tokens)
    key_grad, value_grad, parts = finish(
        place, carried.reshape(-1, DH, DH), states, keys, values, log_decay, inner, inputs, devices
    )
    near = exchanged(parts, ("z",), ("x",))
    near = summed(near_kernel, near, pltpu.VMEM(parts.shape[1:], BF16), "near")
    far = exchanged(near, ("x", "y"), ("z", "y"))
    out = jax.ShapeDtypeStruct((parts.shape[2] // 2, 2, width), BF16)
    return (key_grad, value_grad, summed(far_kernel, far, out, "far"))


def solution(mesh):
    split = Mesh(mesh.devices.reshape(4, 4, 2, 2, 2), EVERY)
    placed = (P(SEQ, TP),) * 4 + (P(None, SEQ), P(SEQ, None))
    return jax.shard_map(
        shards,
        mesh=split,
        in_specs=placed,
        out_specs=(P(SEQ, TP), P(SEQ, TP), P(SEQ, None, TP)),
        check_vma=False,
    )
```

```python
import functools
import itertools

import jax
import jax.numpy as jnp
from jax import lax
from jax.experimental import pallas as pl
from jax.experimental.pallas import tpu as pltpu
from jax.sharding import Mesh
from jax.sharding import PartitionSpec as P

DH = 256
BLOCK = 512
SEQ = ("z", "x", "y")
TP = ("lo", "core")
EVERY = SEQ + TP
F32 = jnp.float32
BF16 = jnp.bfloat16
SCALE = DH ** (-0.5)


def cumulate(rows):
    lane = lax.rem(lax.broadcasted_iota(jnp.int32, rows.shape, 1), BLOCK)
    step = 1
    while step < BLOCK:
        rows = rows + jnp.where(lane >= step, pltpu.roll(rows, step, 1), 0.0)
        step *= 2
    return rows


def own_rows(rows, first, heads):
    index = lax.broadcasted_iota(jnp.int32, rows.shape, 0)
    picked = [jnp.sum(jnp.where(index == first + h, rows, 0.0), axis=0, keepdims=True) for h in range(heads)]
    out = jnp.zeros_like(rows)
    for h in range(heads):
        out = jnp.where(index == h, picked[h], out)
    return out


def dot_tt(a, b):
    return lax.dot_general(a, b, (((0,), (0,)), ((), ())), preferred_element_type=F32)


def dot_nt(a, b):
    return lax.dot_general(a, b, (((1,), (1,)), ((), ())), preferred_element_type=F32)


def dot_nn(a, b):
    return jnp.dot(a, b, preferred_element_type=F32)


def states_kernel(heads, where_ref, q_ref, g_ref, ld_ref, state_ref, message_ref, total, passed):
    block = pl.program_id(0)

    @pl.when(block == 0)
    def _():
        total[...] = jnp.zeros_like(total)
        passed[...] = jnp.zeros_like(passed)

    cum = cumulate(own_rows(ld_ref[...], where_ref[0] * heads, heads))
    decay = (SCALE * jnp.exp(cum)).T
    before = passed[:, 0:1]
    sums = [total[h] for h in range(heads)]
    for c in range(state_ref.shape[0]):
        rows = slice(c * BLOCK, (c + 1) * BLOCK)
        kept = jnp.exp(before)
        for h in range(heads):
            cols = slice(h * DH, (h + 1) * DH)
            weighted = (q_ref[rows, cols].astype(F32) * decay[rows, h : h + 1]).astype(BF16)
            state = dot_tt(weighted, g_ref[rows, cols])
            state_ref[c, h] = state
            sums[h] = sums[h] + kept[h : h + 1, :] * state
        before = before + cum[:, (c + 1) * BLOCK - 1 : (c + 1) * BLOCK]
    for h in range(heads):
        total[h] = sums[h]
    passed[...] = jnp.broadcast_to(before, passed.shape)

    @pl.when(block == pl.num_programs(0) - 1)
    def _():
        piece = message_ref.shape[1]
        each = DH // piece
        row = lax.broadcasted_iota(jnp.int32, (piece, 128), 0)
        for h in range(heads):
            gone = jnp.broadcast_to(passed[h : h + 1, :], (piece, 128))
            high = gone.astype(BF16).astype(F32)
            middle = (gone - high).astype(BF16).astype(F32)
            low = gone - high - middle
            tail = jnp.where(row == 0, high, jnp.where(row == 1, middle, jnp.where(row == 2, low, 0.0)))
            tail = tail.astype(BF16)
            for k in range(each):
                message_ref[h * each + k, :, :DH] = total[h, k * piece : (k + 1) * piece, :].astype(BF16)
                message_ref[h * each + k, :, DH:] = tail


def block_states(place, queries, out_grad, log_decay, devices):
    rows, width = queries.shape
    heads = width // DH
    blocks = rows // BLOCK
    piece = heads * DH // devices
    per = 2
    return pl.pallas_call(
        functools.partial(states_kernel, heads),
        grid_spec=pltpu.PrefetchScalarGridSpec(
            num_scalar_prefetch=1,
            grid=(blocks // per,),
            in_specs=[
                pl.BlockSpec((per * BLOCK, width), lambda i, s: (i, 0)),
                pl.BlockSpec((per * BLOCK, width), lambda i, s: (i, 0)),
                pl.BlockSpec((log_decay.shape[0], per * BLOCK), lambda i, s: (0, i)),
            ],
            out_specs=[
                pl.BlockSpec((per, heads, DH, DH), lambda i, s: (i, 0, 0, 0)),
                pl.BlockSpec((devices, piece, DH + 128), lambda i, s: (0, 0, 0)),
            ],
            scratch_shapes=[pltpu.VMEM((heads, DH, DH), F32), pltpu.VMEM((log_decay.shape[0], 128), F32)],
        ),
        out_shape=[
            jax.ShapeDtypeStruct((blocks, heads, DH, DH), F32),
            pltpu.VMEM((devices, piece, DH + 128), BF16),
        ],
        cost_estimate=pl.CostEstimate(
            flops=2 * rows * width * DH, bytes_accessed=4 * rows * width + 4 * blocks * width * DH, transcendentals=rows
        ),
        name="states",
    )(place, queries, out_grad, log_decay)


def chain_kernel(message_ref, out_ref):
    devices, piece, _ = message_ref.shape
    carried = jnp.zeros((piece, DH), F32)
    for d in reversed(range(devices)):
        out_ref[d] = carried.astype(BF16)
        logs = jnp.sum(message_ref[d, :, DH:].astype(F32), axis=0, keepdims=True)
        gamma = jnp.exp(logs)
        gamma = jnp.concatenate([gamma] * (DH // 128), axis=1)
        carried = message_ref[d, :, :DH].astype(F32) + gamma * carried


def chain(message):
    devices, piece, _ = message.shape
    return pl.pallas_call(
        chain_kernel,
        out_shape=pltpu.VMEM((devices, piece, DH), BF16),
        cost_estimate=pl.CostEstimate(flops=4 * devices * piece * DH, bytes_accessed=4 * message.size, transcendentals=0),
        compiler_params=pltpu.CompilerParams(vmem_limit_bytes=8 << 20),
        name="chain",
    )(message)


def inside_kernel(heads, head, where_ref, q_ref, k_ref, v_ref, g_ref, ld_ref, ik_ref, iv_ref):
    cum = cumulate(own_rows(ld_ref[...], where_ref[0] * heads, heads))
    columns = cum.T
    half = BLOCK // 2
    row = lax.broadcasted_iota(jnp.int32, (half, half), 0)
    column = lax.broadcasted_iota(jnp.int32, (half, half), 1)
    seen = row >= column
    for c in range(q_ref.shape[0] // BLOCK):
        for j in range(2):
            sources = slice(c * BLOCK + j * half, c * BLOCK + (j + 1) * half)
            k, v = (k_ref[sources, :], v_ref[sources, :])
            key_part = value_part = None
            for i in range(j, 2):
                targets = slice(c * BLOCK + i * half, c * BLOCK + (i + 1) * half)
                q, g = (q_ref[targets, :], g_ref[targets, :])
                spread = columns[targets, head : head + 1] - cum[head : head + 1, sources]
                weights = SCALE * jnp.exp(jnp.minimum(spread, 0.0))
                if i == j:
                    weights = jnp.where(seen, weights, 0.0)
                key_scores = (dot_nt(q, k) * weights).astype(BF16)
                grad_scores = (dot_nt(g, v) * weights).astype(BF16)
                to_key, to_value = (dot_tt(grad_scores, q), dot_tt(key_scores, g))
                key_part = to_key if key_part is None else key_part + to_key
                value_part = to_value if value_part is None else value_part + to_value
            ik_ref[sources, :] = key_part.astype(BF16)
            iv_ref[sources, :] = value_part.astype(BF16)


def inside(place, head, queries, keys, values, out_grad, log_decay):
    rows, width = queries.shape
    heads = width // DH
    per = 2 * BLOCK
    tokens = pl.BlockSpec((per, DH), lambda i, s: (i, head))
    return pl.pallas_call(
        functools.partial(inside_kernel, heads, head),
        grid_spec=pltpu.PrefetchScalarGridSpec(
            num_scalar_prefetch=1,
            grid=(rows // per,),
            in_specs=[tokens] * 4 + [pl.BlockSpec((log_decay.shape[0], per), lambda i, s: (0, i))],
            out_specs=[pl.BlockSpec((per, DH), lambda i, s: (i, 0))] * 2,
        ),
        out_shape=[jax.ShapeDtypeStruct((rows, DH), BF16)] * 2,
        cost_estimate=pl.CostEstimate(
            flops=8 * rows * DH * BLOCK, bytes_accessed=12 * rows * DH, transcendentals=rows * BLOCK
        ),
        name=f"inside{head}",
    )(place, queries, keys, values, out_grad, log_decay)


def finish_kernel(heads, steps, where_ref, c_ref, state_ref, k_ref, v_ref, ld_ref, *refs):
    inner = refs[: 2 * heads]
    *x_refs, kg_ref, vg_ref, out_ref, carry, grads = refs[2 * heads :]
    step = pl.program_id(0)
    width = heads * DH
    per = state_ref.shape[0]

    @pl.when(step == 0)
    def _():
        carry[...] = c_ref[...].astype(F32)

    @pl.when(step < steps)
    def _():
        cum = cumulate(own_rows(ld_ref[...], where_ref[0] * heads, heads))
        lasts = [cum[:, (c + 1) * BLOCK - 1 : (c + 1) * BLOCK] for c in range(per)]
        base = jnp.concatenate([jnp.broadcast_to(last, (cum.shape[0], BLOCK)) for last in lasts], axis=1)
        decayed = jnp.exp(base - cum).T
        carries = [carry[h] for h in range(heads)]
        for c in reversed(range(per)):
            here = slice(c * BLOCK, (c + 1) * BLOCK)
            there = pl.ds(pl.multiple_of(((steps - 1 - step) * per + c) * BLOCK, BLOCK), BLOCK)
            kept = jnp.exp(lasts[c])
            for h in range(heads):
                cols = slice(h * DH, (h + 1) * DH)
                low = carries[h].astype(BF16)
                over = decayed[here, h : h + 1]
                key_grad = (inner[2 * h][here, :].astype(F32) + over * dot_nt(v_ref[here, cols], low)).astype(BF16)
                value_grad = (inner[2 * h + 1][here, :].astype(F32) + over * dot_nn(k_ref[here, cols], low)).astype(BF16)
                kg_ref[here, cols] = key_grad
                vg_ref[here, cols] = value_grad
                grads[there, cols] = key_grad
                grads[there, width + h * DH : width + (h + 1) * DH] = value_grad
                carries[h] = kept[h : h + 1, :] * carries[h] + state_ref[c, h]
        for h in range(heads):
            carry[h] = carries[h]

    @pl.when(step >= steps)
    def _():
        slots, share, _ = out_ref.shape[1:]
        share = share // 2
        x = jnp.concatenate([ref[...] for ref in x_refs], axis=1)
        for part in range(2):
            sums = dot_tt(x, grads[:, part * width : (part + 1) * width]).astype(BF16)
            for d in range(slots):
                out_ref[0, d, part * share : (part + 1) * share, :] = sums[d * share : (d + 1) * share, :]


def finish(place, carried, states, keys, values, log_decay, inner, inputs, devices):
    rows, width = keys.shape
    heads = width // DH
    blocks = rows // BLOCK
    per = 2
    steps = blocks // per
    wide = inputs.shape[1]
    share = wide // devices

    def back(i):
        return jnp.maximum(steps - 1 - i, 0)

    def later(i):
        return jnp.maximum(i - steps, 0)

    def columns(k):
        return pl.BlockSpec(
            (rows, wide // 16),
            lambda i, s: (0, jnp.where(lax.rem(s[0], 2) == 0, 4 * later(i) + k, 4 * k + later(i))),
        )

    tokens = pl.BlockSpec((per * BLOCK, width), lambda i, s: (back(i), 0))
    return pl.pallas_call(
        functools.partial(finish_kernel, heads, steps),
        grid_spec=pltpu.PrefetchScalarGridSpec(
            num_scalar_prefetch=1,
            grid=(steps + 4,),
            in_specs=[
                pl.BlockSpec((heads, DH, DH), lambda i, s: (0, 0, 0)),
                pl.BlockSpec((per, heads, DH, DH), lambda i, s: (back(i), 0, 0, 0)),
                tokens,
                tokens,
                pl.BlockSpec((log_decay.shape[0], per * BLOCK), lambda i, s: (0, back(i))),
            ]
            + [pl.BlockSpec((per * BLOCK, DH), lambda i, s: (back(i), 0))] * (2 * heads)
            + [columns(k) for k in range(4)],
            out_specs=[
                tokens,
                tokens,
                pl.BlockSpec((1, devices // 4, 2 * share, width), lambda i, s: (later(i), 0, 0, 0)),
            ],
            scratch_shapes=[pltpu.VMEM((heads, DH, DH), F32), pltpu.VMEM((rows, 2 * width), BF16)],
        ),
        out_shape=[jax.ShapeDtypeStruct((rows, width), BF16)] * 2
        + [pltpu.VMEM((4, devices // 4, 2 * share, width), BF16)],
        cost_estimate=pl.CostEstimate(
            flops=4 * rows * width * (DH + wide), bytes_accessed=16 * rows * width, transcendentals=rows * heads
        ),
        compiler_params=pltpu.CompilerParams(vmem_limit_bytes=48 << 20),
        name="finish",
    )(place, carried, states, keys, values, log_decay, *inner, inputs, inputs, inputs, inputs)


def near_kernel(parts_ref, out_ref):
    rows = 32
    for slot in range(out_ref.shape[0]):
        for at in range(0, out_ref.shape[1], rows):
            total = parts_ref[0, slot, at : at + rows, :].astype(F32)
            for p in range(1, parts_ref.shape[0]):
                total = total + parts_ref[p, slot, at : at + rows, :].astype(F32)
            out_ref[slot, at : at + rows, :] = total.astype(BF16)


def far_kernel(parts_ref, out_ref):
    rows = 16
    share = out_ref.shape[0]
    for start in range(0, parts_ref.shape[1], rows):
        total = parts_ref[0, start : start + rows, :].astype(F32)
        for p in range(1, parts_ref.shape[0]):
            total = total + parts_ref[p, start : start + rows, :].astype(F32)
        at = start % share
        out_ref[at : at + rows, start // share, :] = total.astype(BF16)


def summed(body, parts, shape, name):
    return pl.pallas_call(
        body,
        in_specs=[pl.BlockSpec(memory_space=pltpu.VMEM)],
        out_shape=shape,
        cost_estimate=pl.CostEstimate(flops=parts.size, bytes_accessed=2 * parts.size, transcendentals=0),
        compiler_params=pltpu.CompilerParams(vmem_limit_bytes=12 << 20),
        name=name,
    )(parts)


def groups_of(*axes_of_core):
    sizes = dict(zip(EVERY, (4, 4, 2, 2, 2)))
    out = []
    for core, axes in enumerate(axes_of_core):
        rest = [axis for axis in SEQ + ("lo",) if axis not in axes]
        for fixed in itertools.product(*(range(sizes[axis]) for axis in rest)):
            group = []
            for varied in itertools.product(*(range(sizes[axis]) for axis in axes)):
                spot = dict(zip(rest, fixed)) | dict(zip(axes, varied)) | {"core": core}
                index = 0
                for axis in EVERY:
                    index = index * sizes[axis] + spot[axis]
                group.append(index)
            out.append(group)
    return out


def exchanged(pieces, *axes_of_core):
    return lax.all_to_all(pieces, EVERY, 0, 0, axis_index_groups=groups_of(*axes_of_core), tiled=True)


def shards(queries, keys, values, out_grad, log_decay, inputs):
    devices = lax.axis_size(SEQ)
    width = queries.shape[1]
    place = lax.axis_index(TP).astype(jnp.int32).reshape(1)
    states, message = block_states(place, queries, out_grad, log_decay, devices)
    tokens = (queries, keys, values, out_grad, log_decay)
    arrived = lax.all_to_all(message, SEQ, 0, 0, tiled=True)
    inner = list(inside(place, 0, *tokens))
    arrived, place, *inner = lax.optimization_barrier((arrived, place, *inner))
    carried = lax.all_to_all(chain(arrived), SEQ, 0, 0, tiled=True)
    inner += inside(place, 1, *tokens)
    key_grad, value_grad, parts = finish(
        place, carried.reshape(-1, DH, DH), states, keys, values, log_decay, inner, inputs, devices
    )
    near = exchanged(parts, ("z",), ("x",))
    near = summed(near_kernel, near, pltpu.VMEM(parts.shape[1:], BF16), "near")
    far = exchanged(near, ("x", "y"), ("z", "y"))
    out = jax.ShapeDtypeStruct((parts.shape[2] // 2, 2, width), BF16)
    return (key_grad, value_grad, summed(far_kernel, far, out, "far"))


def solution(mesh):
    split = Mesh(mesh.devices.reshape(4, 4, 2, 2, 2), EVERY)
    placed = (P(SEQ, TP),) * 4 + (P(None, SEQ), P(SEQ, None))
    return jax.shard_map(
        shards,
        mesh=split,
        in_specs=placed,
        out_specs=(P(SEQ, TP), P(SEQ, TP), P(SEQ, None, TP)),
        check_vma=False,
    )
```

```python
import functools
import itertools

import jax
import jax.numpy as jnp
from jax import lax
from jax.experimental import pallas as pl
from jax.experimental.pallas import tpu as pltpu
from jax.sharding import Mesh
from jax.sharding import PartitionSpec as P

DH = 256
BLOCK = 512
SEQ = ("z", "x", "y")
TP = ("lo", "core")
EVERY = SEQ + TP
F32 = jnp.float32
BF16 = jnp.bfloat16
SCALE = DH ** (-0.5)


def cumulate(rows):
    lane = lax.rem(lax.broadcasted_iota(jnp.int32, rows.shape, 1), BLOCK)
    step = 1
    while step < BLOCK:
        rows = rows + jnp.where(lane >= step, pltpu.roll(rows, step, 1), 0.0)
        step *= 2
    return rows


def own_rows(rows, first, heads):
    index = lax.broadcasted_iota(jnp.int32, rows.shape, 0)
    picked = [jnp.sum(jnp.where(index == first + h, rows, 0.0), axis=0, keepdims=True) for h in range(heads)]
    out = jnp.zeros_like(rows)
    for h in range(heads):
        out = jnp.where(index == h, picked[h], out)
    return out


def dot_tt(a, b):
    return lax.dot_general(a, b, (((0,), (0,)), ((), ())), preferred_element_type=F32)


def dot_nt(a, b):
    return lax.dot_general(a, b, (((1,), (1,)), ((), ())), preferred_element_type=F32)


def dot_nn(a, b):
    return jnp.dot(a, b, preferred_element_type=F32)


def states_kernel(heads, where_ref, q_ref, g_ref, ld_ref, state_ref, message_ref, total, passed):
    block = pl.program_id(0)

    @pl.when(block == 0)
    def _():
        total[...] = jnp.zeros_like(total)
        passed[...] = jnp.zeros_like(passed)

    cum = cumulate(own_rows(ld_ref[...], where_ref[0] * heads, heads))
    decay = (SCALE * jnp.exp(cum)).T
    before = passed[:, 0:1]
    sums = [total[h] for h in range(heads)]
    for c in range(state_ref.shape[0]):
        rows = slice(c * BLOCK, (c + 1) * BLOCK)
        kept = jnp.exp(before)
        for h in range(heads):
            cols = slice(h * DH, (h + 1) * DH)
            weighted = (q_ref[rows, cols].astype(F32) * decay[rows, h : h + 1]).astype(BF16)
            state = dot_tt(weighted, g_ref[rows, cols])
            state_ref[c, h] = state
            sums[h] = sums[h] + kept[h : h + 1, :] * state
        before = before + cum[:, (c + 1) * BLOCK - 1 : (c + 1) * BLOCK]
    for h in range(heads):
        total[h] = sums[h]
    passed[...] = jnp.broadcast_to(before, passed.shape)

    @pl.when(block == pl.num_programs(0) - 1)
    def _():
        piece = message_ref.shape[1]
        each = DH // piece
        row = lax.broadcasted_iota(jnp.int32, (piece, 128), 0)
        for h in range(heads):
            gone = jnp.broadcast_to(passed[h : h + 1, :], (piece, 128))
            high = gone.astype(BF16).astype(F32)
            middle = (gone - high).astype(BF16).astype(F32)
            low = gone - high - middle
            tail = jnp.where(row == 0, high, jnp.where(row == 1, middle, jnp.where(row == 2, low, 0.0)))
            tail = tail.astype(BF16)
            for k in range(each):
                message_ref[h * each + k, :, :DH] = total[h, k * piece : (k + 1) * piece, :].astype(BF16)
                message_ref[h * each + k, :, DH:] = tail


def block_states(place, queries, out_grad, log_decay, devices):
    rows, width = queries.shape
    heads = width // DH
    blocks = rows // BLOCK
    piece = heads * DH // devices
    per = 2
    return pl.pallas_call(
        functools.partial(states_kernel, heads),
        grid_spec=pltpu.PrefetchScalarGridSpec(
            num_scalar_prefetch=1,
            grid=(blocks // per,),
            in_specs=[
                pl.BlockSpec((per * BLOCK, width), lambda i, s: (i, 0)),
                pl.BlockSpec((per * BLOCK, width), lambda i, s: (i, 0)),
                pl.BlockSpec((log_decay.shape[0], per * BLOCK), lambda i, s: (0, i)),
            ],
            out_specs=[
                pl.BlockSpec((per, heads, DH, DH), lambda i, s: (i, 0, 0, 0)),
                pl.BlockSpec((devices, piece, DH + 128), lambda i, s: (0, 0, 0)),
            ],
            scratch_shapes=[pltpu.VMEM((heads, DH, DH), F32), pltpu.VMEM((log_decay.shape[0], 128), F32)],
        ),
        out_shape=[
            jax.ShapeDtypeStruct((blocks, heads, DH, DH), F32),
            pltpu.VMEM((devices, piece, DH + 128), BF16),
        ],
        cost_estimate=pl.CostEstimate(
            flops=2 * rows * width * DH, bytes_accessed=4 * rows * width + 4 * blocks * width * DH, transcendentals=rows
        ),
        name="states",
    )(place, queries, out_grad, log_decay)


def chain_kernel(message_ref, out_ref):
    devices, piece, _ = message_ref.shape
    carried = jnp.zeros((piece, DH), F32)
    for d in reversed(range(devices)):
        out_ref[d] = carried.astype(BF16)
        logs = jnp.sum(message_ref[d, :, DH:].astype(F32), axis=0, keepdims=True)
        gamma = jnp.exp(logs)
        gamma = jnp.concatenate([gamma] * (DH // 128), axis=1)
        carried = message_ref[d, :, :DH].astype(F32) + gamma * carried


def chain(message):
    devices, piece, _ = message.shape
    return pl.pallas_call(
        chain_kernel,
        out_shape=pltpu.VMEM((devices, piece, DH), BF16),
        cost_estimate=pl.CostEstimate(flops=4 * devices * piece * DH, bytes_accessed=4 * message.size, transcendentals=0),
        compiler_params=pltpu.CompilerParams(vmem_limit_bytes=8 << 20),
        name="chain",
    )(message)


def inside_kernel(heads, head, where_ref, q_ref, k_ref, v_ref, g_ref, ld_ref, ik_ref, iv_ref):
    cum = cumulate(own_rows(ld_ref[...], where_ref[0] * heads, heads))
    columns = cum.T
    half = BLOCK // 2
    row = lax.broadcasted_iota(jnp.int32, (half, half), 0)
    column = lax.broadcasted_iota(jnp.int32, (half, half), 1)
    seen = column >= row
    for c in range(q_ref.shape[0] // BLOCK):
        for j in range(2):
            sources = slice(c * BLOCK + j * half, c * BLOCK + (j + 1) * half)
            k, v = (k_ref[sources, :], v_ref[sources, :])
            key_part = value_part = None
            for i in range(j, 2):
                targets = slice(c * BLOCK + i * half, c * BLOCK + (i + 1) * half)
                q, g = (q_ref[targets, :], g_ref[targets, :])
                spread = cum[head : head + 1, targets] - columns[sources, head : head + 1]
                weights = SCALE * jnp.exp(jnp.minimum(spread, 0.0))
                if i == j:
                    weights = jnp.where(seen, weights, 0.0)
                key_scores = (dot_nt(k, q) * weights).astype(BF16)
                grad_scores = (dot_nt(v, g) * weights).astype(BF16)
                to_key, to_value = (dot_nn(grad_scores, q), dot_nn(key_scores, g))
                key_part = to_key if key_part is None else key_part + to_key
                value_part = to_value if value_part is None else value_part + to_value
            ik_ref[sources, :] = key_part.astype(BF16)
            iv_ref[sources, :] = value_part.astype(BF16)


def inside(place, head, queries, keys, values, out_grad, log_decay):
    rows, width = queries.shape
    heads = width // DH
    per = 2 * BLOCK
    tokens = pl.BlockSpec((per, DH), lambda i, s: (i, head))
    return pl.pallas_call(
        functools.partial(inside_kernel, heads, head),
        grid_spec=pltpu.PrefetchScalarGridSpec(
            num_scalar_prefetch=1,
            grid=(rows // per,),
            in_specs=[tokens] * 4 + [pl.BlockSpec((log_decay.shape[0], per), lambda i, s: (0, i))],
            out_specs=[pl.BlockSpec((per, DH), lambda i, s: (i, 0))] * 2,
        ),
        out_shape=[jax.ShapeDtypeStruct((rows, DH), BF16)] * 2,
        cost_estimate=pl.CostEstimate(
            flops=8 * rows * DH * BLOCK, bytes_accessed=12 * rows * DH, transcendentals=rows * BLOCK
        ),
        name=f"inside{head}",
    )(place, queries, keys, values, out_grad, log_decay)


def finish_kernel(heads, steps, where_ref, c_ref, state_ref, k_ref, v_ref, ld_ref, *refs):
    inner = refs[: 2 * heads]
    *x_refs, kg_ref, vg_ref, out_ref, carry, grads = refs[2 * heads :]
    step = pl.program_id(0)
    width = heads * DH
    per = state_ref.shape[0]

    @pl.when(step == 0)
    def _():
        carry[...] = c_ref[...].astype(F32)

    @pl.when(step < steps)
    def _():
        cum = cumulate(own_rows(ld_ref[...], where_ref[0] * heads, heads))
        lasts = [cum[:, (c + 1) * BLOCK - 1 : (c + 1) * BLOCK] for c in range(per)]
        base = jnp.concatenate([jnp.broadcast_to(last, (cum.shape[0], BLOCK)) for last in lasts], axis=1)
        decayed = jnp.exp(base - cum).T
        carries = [carry[h] for h in range(heads)]
        for c in reversed(range(per)):
            here = slice(c * BLOCK, (c + 1) * BLOCK)
            there = pl.ds(pl.multiple_of(((steps - 1 - step) * per + c) * BLOCK, BLOCK), BLOCK)
            kept = jnp.exp(lasts[c])
            for h in range(heads):
                cols = slice(h * DH, (h + 1) * DH)
                low = carries[h].astype(BF16)
                over = decayed[here, h : h + 1]
                key_grad = (inner[2 * h][here, :].astype(F32) + over * dot_nt(v_ref[here, cols], low)).astype(BF16)
                value_grad = (inner[2 * h + 1][here, :].astype(F32) + over * dot_nn(k_ref[here, cols], low)).astype(BF16)
                kg_ref[here, cols] = key_grad
                vg_ref[here, cols] = value_grad
                grads[there, cols] = key_grad
                grads[there, width + h * DH : width + (h + 1) * DH] = value_grad
                carries[h] = kept[h : h + 1, :] * carries[h] + state_ref[c, h]
        for h in range(heads):
            carry[h] = carries[h]

    @pl.when(step >= steps)
    def _():
        slots, share, _ = out_ref.shape[1:]
        share = share // 2
        x = jnp.concatenate([ref[...] for ref in x_refs], axis=1)
        for part in range(2):
            sums = dot_tt(x, grads[:, part * width : (part + 1) * width]).astype(BF16)
            for d in range(slots):
                out_ref[0, d, part * share : (part + 1) * share, :] = sums[d * share : (d + 1) * share, :]


def finish(place, carried, states, keys, values, log_decay, inner, inputs, devices):
    rows, width = keys.shape
    heads = width // DH
    blocks = rows // BLOCK
    per = 2
    steps = blocks // per
    wide = inputs.shape[1]
    share = wide // devices

    def back(i):
        return jnp.maximum(steps - 1 - i, 0)

    def later(i):
        return jnp.maximum(i - steps, 0)

    def columns(k):
        return pl.BlockSpec(
            (rows, wide // 16),
            lambda i, s: (0, jnp.where(lax.rem(s[0], 2) == 0, 4 * later(i) + k, 4 * k + later(i))),
        )

    tokens = pl.BlockSpec((per * BLOCK, width), lambda i, s: (back(i), 0))
    return pl.pallas_call(
        functools.partial(finish_kernel, heads, steps),
        grid_spec=pltpu.PrefetchScalarGridSpec(
            num_scalar_prefetch=1,
            grid=(steps + 4,),
            in_specs=[
                pl.BlockSpec((heads, DH, DH), lambda i, s: (0, 0, 0)),
                pl.BlockSpec((per, heads, DH, DH), lambda i, s: (back(i), 0, 0, 0)),
                tokens,
                tokens,
                pl.BlockSpec((log_decay.shape[0], per * BLOCK), lambda i, s: (0, back(i))),
            ]
            + [pl.BlockSpec((per * BLOCK, DH), lambda i, s: (back(i), 0))] * (2 * heads)
            + [columns(k) for k in range(4)],
            out_specs=[
                tokens,
                tokens,
                pl.BlockSpec((1, devices // 4, 2 * share, width), lambda i, s: (later(i), 0, 0, 0)),
            ],
            scratch_shapes=[pltpu.VMEM((heads, DH, DH), F32), pltpu.VMEM((rows, 2 * width), BF16)],
        ),
        out_shape=[jax.ShapeDtypeStruct((rows, width), BF16)] * 2
        + [pltpu.VMEM((4, devices // 4, 2 * share, width), BF16)],
        cost_estimate=pl.CostEstimate(
            flops=4 * rows * width * (DH + wide), bytes_accessed=16 * rows * width, transcendentals=rows * heads
        ),
        compiler_params=pltpu.CompilerParams(vmem_limit_bytes=48 << 20),
        name="finish",
    )(place, carried, states, keys, values, log_decay, *inner, inputs, inputs, inputs, inputs)


def near_kernel(parts_ref, out_ref):
    rows = 32
    for slot in range(out_ref.shape[0]):
        for at in range(0, out_ref.shape[1], rows):
            total = parts_ref[0, slot, at : at + rows, :].astype(F32)
            for p in range(1, parts_ref.shape[0]):
                total = total + parts_ref[p, slot, at : at + rows, :].astype(F32)
            out_ref[slot, at : at + rows, :] = total.astype(BF16)


def far_kernel(parts_ref, out_ref):
    rows = 16
    share = out_ref.shape[0]
    for start in range(0, parts_ref.shape[1], rows):
        total = parts_ref[0, start : start + rows, :].astype(F32)
        for p in range(1, parts_ref.shape[0]):
            total = total + parts_ref[p, start : start + rows, :].astype(F32)
        at = start % share
        out_ref[at : at + rows, start // share, :] = total.astype(BF16)


def summed(body, parts, shape, name):
    return pl.pallas_call(
        body,
        in_specs=[pl.BlockSpec(memory_space=pltpu.VMEM)],
        out_shape=shape,
        cost_estimate=pl.CostEstimate(flops=parts.size, bytes_accessed=2 * parts.size, transcendentals=0),
        compiler_params=pltpu.CompilerParams(vmem_limit_bytes=12 << 20),
        name=name,
    )(parts)


def groups_of(*axes_of_core):
    sizes = dict(zip(EVERY, (4, 4, 2, 2, 2)))
    out = []
    for core, axes in enumerate(axes_of_core):
        rest = [axis for axis in SEQ + ("lo",) if axis not in axes]
        for fixed in itertools.product(*(range(sizes[axis]) for axis in rest)):
            group = []
            for varied in itertools.product(*(range(sizes[axis]) for axis in axes)):
                spot = dict(zip(rest, fixed)) | dict(zip(axes, varied)) | {"core": core}
                index = 0
                for axis in EVERY:
                    index = index * sizes[axis] + spot[axis]
                group.append(index)
            out.append(group)
    return out


def exchanged(pieces, *axes_of_core):
    return lax.all_to_all(pieces, EVERY, 0, 0, axis_index_groups=groups_of(*axes_of_core), tiled=True)


def shards(queries, keys, values, out_grad, log_decay, inputs):
    devices = lax.axis_size(SEQ)
    width = queries.shape[1]
    place = lax.axis_index(TP).astype(jnp.int32).reshape(1)
    states, message = block_states(place, queries, out_grad, log_decay, devices)
    tokens = (queries, keys, values, out_grad, log_decay)
    arrived = lax.all_to_all(message, SEQ, 0, 0, tiled=True)
    inner = list(inside(place, 0, *tokens))
    arrived, place, *inner = lax.optimization_barrier((arrived, place, *inner))
    carried = lax.all_to_all(chain(arrived), SEQ, 0, 0, tiled=True)
    inner += inside(place, 1, *tokens)
    key_grad, value_grad, parts = finish(
        place, carried.reshape(-1, DH, DH), states, keys, values, log_decay, inner, inputs, devices
    )
    near = exchanged(parts, ("z",), ("x",))
    near = summed(near_kernel, near, pltpu.VMEM(parts.shape[1:], BF16), "near")
    far = exchanged(near, ("x", "y"), ("z", "y"))
    out = jax.ShapeDtypeStruct((parts.shape[2] // 2, 2, width), BF16)
    return (key_grad, value_grad, summed(far_kernel, far, out, "far"))


def solution(mesh):
    split = Mesh(mesh.devices.reshape(4, 4, 2, 2, 2), EVERY)
    placed = (P(SEQ, TP),) * 4 + (P(None, SEQ), P(SEQ, None))
    return jax.shard_map(
        shards,
        mesh=split,
        in_specs=placed,
        out_specs=(P(SEQ, TP), P(SEQ, TP), P(SEQ, None, TP)),
        check_vma=False,
    )
```

```python
import functools
import itertools

import jax
import jax.numpy as jnp
from jax import lax
from jax.experimental import pallas as pl
from jax.experimental.pallas import tpu as pltpu
from jax.sharding import Mesh
from jax.sharding import PartitionSpec as P

DH = 256
BLOCK = 512
SEQ = ("z", "x", "y")
TP = ("lo", "core")
EVERY = SEQ + TP
F32 = jnp.float32
BF16 = jnp.bfloat16
SCALE = DH ** (-0.5)


def cumulate(rows):
    lane = lax.rem(lax.broadcasted_iota(jnp.int32, rows.shape, 1), BLOCK)
    step = 1
    while step < BLOCK:
        rows = rows + jnp.where(lane >= step, pltpu.roll(rows, step, 1), 0.0)
        step *= 2
    return rows


def own_rows(rows, first, heads):
    index = lax.broadcasted_iota(jnp.int32, rows.shape, 0)
    picked = [jnp.sum(jnp.where(index == first + h, rows, 0.0), axis=0, keepdims=True) for h in range(heads)]
    out = jnp.zeros_like(rows)
    for h in range(heads):
        out = jnp.where(index == h, picked[h], out)
    return out


def dot_tt(a, b):
    return lax.dot_general(a, b, (((0,), (0,)), ((), ())), preferred_element_type=F32)


def dot_nt(a, b):
    return lax.dot_general(a, b, (((1,), (1,)), ((), ())), preferred_element_type=F32)


def dot_nn(a, b):
    return jnp.dot(a, b, preferred_element_type=F32)


def states_kernel(heads, where_ref, q_ref, g_ref, ld_ref, state_ref, message_ref, total, passed):
    block = pl.program_id(0)

    @pl.when(block == 0)
    def _():
        total[...] = jnp.zeros_like(total)
        passed[...] = jnp.zeros_like(passed)

    cum = cumulate(own_rows(ld_ref[...], where_ref[0] * heads, heads))
    decay = SCALE * jnp.exp(cum)
    before = passed[:, 0:1]
    sums = [total[h] for h in range(heads)]
    for c in range(state_ref.shape[0]):
        rows = slice(c * BLOCK, (c + 1) * BLOCK)
        kept = jnp.exp(before)
        for h in range(heads):
            cols = slice(h * DH, (h + 1) * DH)
            weighted = (q_ref[rows, cols].T.astype(F32) * decay[h : h + 1, rows]).astype(BF16)
            state = dot_nn(weighted, g_ref[rows, cols])
            state_ref[c, h] = state
            sums[h] = sums[h] + kept[h : h + 1, :] * state
        before = before + cum[:, (c + 1) * BLOCK - 1 : (c + 1) * BLOCK]
    for h in range(heads):
        total[h] = sums[h]
    passed[...] = jnp.broadcast_to(before, passed.shape)

    @pl.when(block == pl.num_programs(0) - 1)
    def _():
        piece = message_ref.shape[1]
        each = DH // piece
        row = lax.broadcasted_iota(jnp.int32, (piece, 128), 0)
        for h in range(heads):
            gone = jnp.broadcast_to(passed[h : h + 1, :], (piece, 128))
            high = gone.astype(BF16).astype(F32)
            middle = (gone - high).astype(BF16).astype(F32)
            low = gone - high - middle
            tail = jnp.where(row == 0, high, jnp.where(row == 1, middle, jnp.where(row == 2, low, 0.0)))
            tail = tail.astype(BF16)
            for k in range(each):
                message_ref[h * each + k, :, :DH] = total[h, k * piece : (k + 1) * piece, :].astype(BF16)
                message_ref[h * each + k, :, DH:] = tail


def block_states(place, queries, out_grad, log_decay, devices):
    rows, width = queries.shape
    heads = width // DH
    blocks = rows // BLOCK
    piece = heads * DH // devices
    per = 2
    return pl.pallas_call(
        functools.partial(states_kernel, heads),
        grid_spec=pltpu.PrefetchScalarGridSpec(
            num_scalar_prefetch=1,
            grid=(blocks // per,),
            in_specs=[
                pl.BlockSpec((per * BLOCK, width), lambda i, s: (i, 0)),
                pl.BlockSpec((per * BLOCK, width), lambda i, s: (i, 0)),
                pl.BlockSpec((log_decay.shape[0], per * BLOCK), lambda i, s: (0, i)),
            ],
            out_specs=[
                pl.BlockSpec((per, heads, DH, DH), lambda i, s: (i, 0, 0, 0)),
                pl.BlockSpec((devices, piece, DH + 128), lambda i, s: (0, 0, 0)),
            ],
            scratch_shapes=[pltpu.VMEM((heads, DH, DH), F32), pltpu.VMEM((log_decay.shape[0], 128), F32)],
        ),
        out_shape=[
            jax.ShapeDtypeStruct((blocks, heads, DH, DH), F32),
            pltpu.VMEM((devices, piece, DH + 128), BF16),
        ],
        cost_estimate=pl.CostEstimate(
            flops=2 * rows * width * DH, bytes_accessed=4 * rows * width + 4 * blocks * width * DH, transcendentals=rows
        ),
        name="states",
    )(place, queries, out_grad, log_decay)


def chain_kernel(message_ref, out_ref):
    devices, piece, _ = message_ref.shape
    carried = jnp.zeros((piece, DH), F32)
    for d in reversed(range(devices)):
        out_ref[d] = carried.astype(BF16)
        logs = jnp.sum(message_ref[d, :, DH:].astype(F32), axis=0, keepdims=True)
        gamma = jnp.exp(logs)
        gamma = jnp.concatenate([gamma] * (DH // 128), axis=1)
        carried = message_ref[d, :, :DH].astype(F32) + gamma * carried


def chain(message):
    devices, piece, _ = message.shape
    return pl.pallas_call(
        chain_kernel,
        out_shape=pltpu.VMEM((devices, piece, DH), BF16),
        cost_estimate=pl.CostEstimate(flops=4 * devices * piece * DH, bytes_accessed=4 * message.size, transcendentals=0),
        compiler_params=pltpu.CompilerParams(vmem_limit_bytes=8 << 20),
        name="chain",
    )(message)


def inside_kernel(heads, head, where_ref, q_ref, k_ref, v_ref, g_ref, ld_ref, ik_ref, iv_ref):
    cum = cumulate(own_rows(ld_ref[...], where_ref[0] * heads, heads))
    columns = cum.T
    half = BLOCK // 2
    row = lax.broadcasted_iota(jnp.int32, (half, half), 0)
    column = lax.broadcasted_iota(jnp.int32, (half, half), 1)
    seen = column >= row
    for c in range(q_ref.shape[0] // BLOCK):
        for j in range(2):
            sources = slice(c * BLOCK + j * half, c * BLOCK + (j + 1) * half)
            k, v = (k_ref[sources, :], v_ref[sources, :])
            key_part = value_part = None
            for i in range(j, 2):
                targets = slice(c * BLOCK + i * half, c * BLOCK + (i + 1) * half)
                q, g = (q_ref[targets, :], g_ref[targets, :])
                spread = cum[head : head + 1, targets] - columns[sources, head : head + 1]
                weights = SCALE * jnp.exp(jnp.minimum(spread, 0.0))
                if i == j:
                    weights = jnp.where(seen, weights, 0.0)
                key_scores = (dot_nt(k, q) * weights).astype(BF16)
                grad_scores = (dot_nt(v, g) * weights).astype(BF16)
                to_key, to_value = (dot_nn(grad_scores, q), dot_nn(key_scores, g))
                key_part = to_key if key_part is None else key_part + to_key
                value_part = to_value if value_part is None else value_part + to_value
            ik_ref[sources, :] = key_part.astype(BF16)
            iv_ref[sources, :] = value_part.astype(BF16)


def inside(place, head, queries, keys, values, out_grad, log_decay):
    rows, width = queries.shape
    heads = width // DH
    per = 2 * BLOCK
    tokens = pl.BlockSpec((per, DH), lambda i, s: (i, head))
    return pl.pallas_call(
        functools.partial(inside_kernel, heads, head),
        grid_spec=pltpu.PrefetchScalarGridSpec(
            num_scalar_prefetch=1,
            grid=(rows // per,),
            in_specs=[tokens] * 4 + [pl.BlockSpec((log_decay.shape[0], per), lambda i, s: (0, i))],
            out_specs=[pl.BlockSpec((per, DH), lambda i, s: (i, 0))] * 2,
        ),
        out_shape=[jax.ShapeDtypeStruct((rows, DH), BF16)] * 2,
        cost_estimate=pl.CostEstimate(
            flops=8 * rows * DH * BLOCK, bytes_accessed=12 * rows * DH, transcendentals=rows * BLOCK
        ),
        name=f"inside{head}",
    )(place, queries, keys, values, out_grad, log_decay)


def finish_kernel(heads, steps, where_ref, c_ref, state_ref, k_ref, v_ref, ld_ref, *refs):
    inner = refs[: 2 * heads]
    *x_refs, kg_ref, vg_ref, out_ref, carry, grads = refs[2 * heads :]
    step = pl.program_id(0)
    width = heads * DH
    per = state_ref.shape[0]

    @pl.when(step == 0)
    def _():
        carry[...] = c_ref[...].astype(F32)

    @pl.when(step < steps)
    def _():
        cum = cumulate(own_rows(ld_ref[...], where_ref[0] * heads, heads))
        lasts = [cum[:, (c + 1) * BLOCK - 1 : (c + 1) * BLOCK] for c in range(per)]
        base = jnp.concatenate([jnp.broadcast_to(last, (cum.shape[0], BLOCK)) for last in lasts], axis=1)
        decayed = jnp.exp(base - cum).T
        carries = [carry[h] for h in range(heads)]
        for c in reversed(range(per)):
            here = slice(c * BLOCK, (c + 1) * BLOCK)
            there = pl.ds(pl.multiple_of(((steps - 1 - step) * per + c) * BLOCK, BLOCK), BLOCK)
            kept = jnp.exp(lasts[c])
            for h in range(heads):
                cols = slice(h * DH, (h + 1) * DH)
                low = carries[h].astype(BF16)
                over = decayed[here, h : h + 1]
                key_grad = (inner[2 * h][here, :].astype(F32) + over * dot_nt(v_ref[here, cols], low)).astype(BF16)
                value_grad = (inner[2 * h + 1][here, :].astype(F32) + over * dot_nn(k_ref[here, cols], low)).astype(BF16)
                kg_ref[here, cols] = key_grad
                vg_ref[here, cols] = value_grad
                grads[there, cols] = key_grad
                grads[there, width + h * DH : width + (h + 1) * DH] = value_grad
                carries[h] = kept[h : h + 1, :] * carries[h] + state_ref[c, h]
        for h in range(heads):
            carry[h] = carries[h]

    @pl.when(step >= steps)
    def _():
        slots, share, _ = out_ref.shape[1:]
        share = share // 2
        x = jnp.concatenate([ref[...] for ref in x_refs], axis=1)
        for part in range(2):
            sums = dot_tt(x, grads[:, part * width : (part + 1) * width]).astype(BF16)
            for d in range(slots):
                out_ref[0, d, part * share : (part + 1) * share, :] = sums[d * share : (d + 1) * share, :]


def finish(place, carried, states, keys, values, log_decay, inner, inputs, devices):
    rows, width = keys.shape
    heads = width // DH
    blocks = rows // BLOCK
    per = 2
    steps = blocks // per
    wide = inputs.shape[1]
    share = wide // devices

    def back(i):
        return jnp.maximum(steps - 1 - i, 0)

    def later(i):
        return jnp.maximum(i - steps, 0)

    def columns(k):
        return pl.BlockSpec(
            (rows, wide // 16),
            lambda i, s: (0, jnp.where(lax.rem(s[0], 2) == 0, 4 * later(i) + k, 4 * k + later(i))),
        )

    tokens = pl.BlockSpec((per * BLOCK, width), lambda i, s: (back(i), 0))
    return pl.pallas_call(
        functools.partial(finish_kernel, heads, steps),
        grid_spec=pltpu.PrefetchScalarGridSpec(
            num_scalar_prefetch=1,
            grid=(steps + 4,),
            in_specs=[
                pl.BlockSpec((heads, DH, DH), lambda i, s: (0, 0, 0)),
                pl.BlockSpec((per, heads, DH, DH), lambda i, s: (back(i), 0, 0, 0)),
                tokens,
                tokens,
                pl.BlockSpec((log_decay.shape[0], per * BLOCK), lambda i, s: (0, back(i))),
            ]
            + [pl.BlockSpec((per * BLOCK, DH), lambda i, s: (back(i), 0))] * (2 * heads)
            + [columns(k) for k in range(4)],
            out_specs=[
                tokens,
                tokens,
                pl.BlockSpec((1, devices // 4, 2 * share, width), lambda i, s: (later(i), 0, 0, 0)),
            ],
            scratch_shapes=[pltpu.VMEM((heads, DH, DH), F32), pltpu.VMEM((rows, 2 * width), BF16)],
        ),
        out_shape=[jax.ShapeDtypeStruct((rows, width), BF16)] * 2
        + [pltpu.VMEM((4, devices // 4, 2 * share, width), BF16)],
        cost_estimate=pl.CostEstimate(
            flops=4 * rows * width * (DH + wide), bytes_accessed=16 * rows * width, transcendentals=rows * heads
        ),
        compiler_params=pltpu.CompilerParams(vmem_limit_bytes=48 << 20),
        name="finish",
    )(place, carried, states, keys, values, log_decay, *inner, inputs, inputs, inputs, inputs)


def near_kernel(parts_ref, out_ref):
    rows = 32
    for slot in range(out_ref.shape[0]):
        for at in range(0, out_ref.shape[1], rows):
            total = parts_ref[0, slot, at : at + rows, :].astype(F32)
            for p in range(1, parts_ref.shape[0]):
                total = total + parts_ref[p, slot, at : at + rows, :].astype(F32)
            out_ref[slot, at : at + rows, :] = total.astype(BF16)


def far_kernel(parts_ref, out_ref):
    rows = 16
    share = out_ref.shape[0]
    for start in range(0, parts_ref.shape[1], rows):
        total = parts_ref[0, start : start + rows, :].astype(F32)
        for p in range(1, parts_ref.shape[0]):
            total = total + parts_ref[p, start : start + rows, :].astype(F32)
        at = start % share
        out_ref[at : at + rows, start // share, :] = total.astype(BF16)


def summed(body, parts, shape, name):
    return pl.pallas_call(
        body,
        in_specs=[pl.BlockSpec(memory_space=pltpu.VMEM)],
        out_shape=shape,
        cost_estimate=pl.CostEstimate(flops=parts.size, bytes_accessed=2 * parts.size, transcendentals=0),
        compiler_params=pltpu.CompilerParams(vmem_limit_bytes=12 << 20),
        name=name,
    )(parts)


def groups_of(*axes_of_core):
    sizes = dict(zip(EVERY, (4, 4, 2, 2, 2)))
    out = []
    for core, axes in enumerate(axes_of_core):
        rest = [axis for axis in SEQ + ("lo",) if axis not in axes]
        for fixed in itertools.product(*(range(sizes[axis]) for axis in rest)):
            group = []
            for varied in itertools.product(*(range(sizes[axis]) for axis in axes)):
                spot = dict(zip(rest, fixed)) | dict(zip(axes, varied)) | {"core": core}
                index = 0
                for axis in EVERY:
                    index = index * sizes[axis] + spot[axis]
                group.append(index)
            out.append(group)
    return out


def exchanged(pieces, *axes_of_core):
    return lax.all_to_all(pieces, EVERY, 0, 0, axis_index_groups=groups_of(*axes_of_core), tiled=True)


def shards(queries, keys, values, out_grad, log_decay, inputs):
    devices = lax.axis_size(SEQ)
    width = queries.shape[1]
    place = lax.axis_index(TP).astype(jnp.int32).reshape(1)
    states, message = block_states(place, queries, out_grad, log_decay, devices)
    tokens = (queries, keys, values, out_grad, log_decay)
    arrived = lax.all_to_all(message, SEQ, 0, 0, tiled=True)
    inner = list(inside(place, 0, *tokens))
    arrived, place, *inner = lax.optimization_barrier((arrived, place, *inner))
    carried = lax.all_to_all(chain(arrived), SEQ, 0, 0, tiled=True)
    inner += inside(place, 1, *tokens)
    key_grad, value_grad, parts = finish(
        place, carried.reshape(-1, DH, DH), states, keys, values, log_decay, inner, inputs, devices
    )
    near = exchanged(parts, ("z",), ("x",))
    near = summed(near_kernel, near, pltpu.VMEM(parts.shape[1:], BF16), "near")
    far = exchanged(near, ("x", "y"), ("z", "y"))
    out = jax.ShapeDtypeStruct((parts.shape[2] // 2, 2, width), BF16)
    return (key_grad, value_grad, summed(far_kernel, far, out, "far"))


def solution(mesh):
    split = Mesh(mesh.devices.reshape(4, 4, 2, 2, 2), EVERY)
    placed = (P(SEQ, TP),) * 4 + (P(None, SEQ), P(SEQ, None))
    return jax.shard_map(
        shards,
        mesh=split,
        in_specs=placed,
        out_specs=(P(SEQ, TP), P(SEQ, TP), P(SEQ, None, TP)),
        check_vma=False,
    )
```
